32 devices in a mesh: dp: 4 (over y, x), tensor: 8 (over z, core).
Axes of the slice: x: 2, y: 2, z: 4, core: 2. Of those that a mesh axis runs over, the one named last changes fastest.
Arguments:
- logits: bfloat16 [1024, 152064], P('dp', 'tensor'), may hold values from -120 to 256
- child_ids: int32 [1024, 64], P('dp'), may hold values from 0 to 152063
- leaf_counts: int32 [1024, 64], P('dp'), may hold values from 1 to 1024
- leaf_valid: int32 [1024], P('dp'), may hold values from 1 to 64
- leaf_temp: float32 [1024], P('dp'), may hold values from 0.5 to 2
- leaf_owner: int32 [1024], P('dp'), may hold values from 0 to 1023, as said below
Outputs:
- gradient: bfloat16 [1024, 152064], P('dp', 'tensor')
- row_loss: float32 [1024], P('dp')
- mean_loss: float32 [], replicated
The draws below stay inside these ranges and needn't reach their ends.
Inputs may be any that keep to these rules, and one draw needn't show every extreme that they name: `leaf_owner`: every position is named by exactly one leaf row. Of the leaf rows of one dp index, exactly 64 name positions of each owner index.
All inputs are finite; a program needn't handle non-finite values.
Results may differ from the reference program's by a relative error of at most 0.001.
Values may be sent and summed in bfloat16 or wider, within the bound.
No kernel may reach another device: no remote copies, remote signals or barrier semaphores. Data moves between devices by JAX's collectives and lax.ppermute only.
A program may use at most 64 MiB of HBM per device.

```python
import math
import jax
import jax.numpy as jnp
from jax import lax

VOCAB = 152064
CHILD = 64
POS_DEV = 256
POSITIONS = 1024
N_DP = 4


def draw_logits(key, part):
    subkeys = jax.random.split(jax.random.fold_in(key, 7), 3)
    row_index = jnp.arange(POSITIONS, dtype=jnp.float32)
    row_scale = jnp.exp(jax.random.uniform(subkeys[0], (POSITIONS,), minval=0.0, maxval=math.log(3.2))) * (1.0 + 2.0 * row_index / POSITIONS)
    column_scale = jnp.exp(jax.random.uniform(subkeys[1], (VOCAB,), minval=0.0, maxval=math.log(3.2)))
    base_draw = jnp.clip(jax.random.normal(subkeys[2], (POSITIONS, VOCAB)), -4.5, 4.5)
    values = 0.6 * base_draw * row_scale[:, None] * column_scale[None, :]
    return values.astype(jnp.bfloat16)


def draw_leaf_owner(key, part):
    subkeys = jax.random.split(jax.random.fold_in(key, 13), 3)
    block_rows = POS_DEV // N_DP
    shifts = jax.random.permutation(subkeys[0], N_DP).astype(jnp.int32)
    source_dev = jnp.arange(N_DP, dtype=jnp.int32)[:, None]
    slot_index = jnp.arange(POS_DEV, dtype=jnp.int32)[None, :]
    block_index = slot_index // block_rows
    owner_dev = (source_dev + shifts[block_index]) % N_DP
    orders = jax.vmap(lambda subkey: jax.random.permutation(subkey, POS_DEV))(jax.random.split(subkeys[1], N_DP)).astype(jnp.int32)
    local_slot = orders[owner_dev, jnp.broadcast_to(slot_index, (N_DP, POS_DEV))]
    owners = owner_dev * POS_DEV + local_slot
    mixing = jax.vmap(lambda subkey: jax.random.permutation(subkey, POS_DEV))(jax.random.split(subkeys[2], N_DP))
    owners = jnp.take_along_axis(owners, mixing, axis=1)
    return owners.reshape(-1).astype(jnp.int32)


def plant(result, rng, least, high):
    place = [jax.random.randint(jax.random.fold_in(rng, axis), (), 0, length) for axis, length in enumerate(result.shape)]
    main_axis = result.shape.index(max(result.shape))
    neighbour = place[:main_axis] + [(place[main_axis] + 1) % result.shape[main_axis]] + place[main_axis + 1:]
    return result.at[tuple(place)].set(least).at[tuple(neighbour)].set(high)


def level_of(own_key, extent, shards, smallest, high):
    def one(axis_at, blocks):
        draws = jax.random.uniform(jax.random.fold_in(jax.random.fold_in(own_key, 6), axis_at), (blocks,), jnp.float32, smallest / len(shards), high / len(shards))
        return jnp.repeat(jnp.exp(draws), extent[axis_at] // blocks).reshape((-1,) + (1,) * (len(extent) - axis_at - 1))

    gain = one(*shards[0])
    for cut in shards[1:]:
        gain = gain * one(*cut)
    return gain


def setup_inputs(seed: int = 0) -> dict:
    key_list = jax.random.split(jax.random.key(seed), 7)
    return {
        "logits": draw_logits(jax.random.fold_in(key_list[6], 71), 0),
        "child_ids": plant(jax.random.randint(key_list[1], (POSITIONS, CHILD), 0, VOCAB), jax.random.fold_in(key_list[1], 1), 0, VOCAB - 1).astype(jnp.int32),
        "leaf_counts": plant(jax.random.randint(key_list[2], (POSITIONS, CHILD), 1, 1025), jax.random.fold_in(key_list[2], 1), 1, 1024).astype(jnp.int32),
        "leaf_valid": plant(jax.random.randint(key_list[3], (POSITIONS,), 1, CHILD + 1), jax.random.fold_in(key_list[3], 1), 1, CHILD).astype(jnp.int32),
        "leaf_temp": jnp.clip(jnp.exp(math.log(2.0) - 1.3862944 * jax.random.uniform(key_list[4], (POSITIONS,), jnp.float32) ** level_of(key_list[4], (POSITIONS,), ((0, 4),), -0.2, 0.2)), 0.5, 2.0),
        "leaf_owner": draw_leaf_owner(jax.random.fold_in(key_list[6], 71), 0),
    }


def reference(logits, child_ids, leaf_counts, leaf_valid, leaf_temp, leaf_owner):
    slot_index = jnp.arange(CHILD, dtype=jnp.int32)
    in_use = slot_index[None, :] < leaf_valid[:, None]
    powered = jnp.exp(jnp.log(leaf_counts.astype(jnp.float32)) * leaf_temp[:, None])
    weights = jnp.where(in_use, powered, jnp.float32(0.0))
    placed = jnp.zeros((POSITIONS, CHILD), jnp.float32).at[leaf_owner].add(weights)
    targets = placed / jnp.sum(placed, axis=1)[:, None]

    def per_block(pieces):
        block_logits, block_targets, block_ids = pieces
        values = block_logits.astype(jnp.float32)
        row_top = jnp.max(values, axis=1)
        shifted = jnp.exp(values - row_top[:, None])
        sumexp = jnp.sum(shifted, axis=1)
        picked = jnp.sum(block_targets * jnp.take_along_axis(values, block_ids, axis=1), axis=1)
        losses = row_top + jnp.log(sumexp) - picked
        row_index = jnp.arange(block_ids.shape[0], dtype=jnp.int32)[:, None]
        target_dense = jnp.zeros_like(values).at[row_index, block_ids].add(block_targets)
        gradient = (shifted / sumexp[:, None] - target_dense).astype(jnp.bfloat16)
        return gradient, losses

    gradient, losses = lax.map(per_block, (logits.reshape(N_DP, POS_DEV, VOCAB), targets.reshape(N_DP, POS_DEV, CHILD), child_ids.reshape(N_DP, POS_DEV, CHILD)))
    row_loss = losses.reshape(POSITIONS)
    mean_loss = jnp.sum(row_loss) / POSITIONS
    return gradient.reshape(POSITIONS, VOCAB), row_loss, mean_loss
```

```python
import functools
import math

import jax
import jax.numpy as jnp
from jax import lax
from jax.experimental import pallas as pl
from jax.experimental.pallas import tpu as pltpu
from jax.sharding import PartitionSpec as P

LOG2E = 1.4426950408889634
LANE_ROWS = 16
DEPTH = 3
VMEM_BYTES = 48 * 1024 * 1024


def largest_block(rows, limit):
    units = rows // LANE_ROWS
    best = 1
    for size in range(1, units + 1):
        if units % size == 0 and size * LANE_ROWS <= limit:
            best = size
    return best * LANE_ROWS


def any_spec():
    return pl.BlockSpec(memory_space=pl.ANY)


def vmem_spec():
    return pl.BlockSpec(memory_space=pltpu.VMEM)


def smem_spec():
    return pl.BlockSpec(memory_space=pltpu.SMEM)


def prepare_kernel(counts_ref, valid_ref, temp_ref, owner_ref, out_ref):
    children, rows = counts_ref.shape
    slot = lax.broadcasted_iota(jnp.int32, (children, rows), 0)
    powered = jnp.exp(jnp.log(counts_ref[...].astype(jnp.float32)) * temp_ref[...])
    weights = jnp.where(slot < valid_ref[...], powered, 0.0)
    out_ref[:children, :] = weights / jnp.sum(weights, axis=0, keepdims=True)
    extra = out_ref.shape[0] - children
    out_ref[children:, :] = jnp.broadcast_to(owner_ref[...].astype(jnp.float32), (extra, rows))


def chunk_copies(x_hbm, x_ref, sems, chunk):
    def copy(index):
        window = pl.ds(index * chunk, chunk)
        return pltpu.make_async_copy(x_hbm.at[window, :], x_ref.at[window, :], sems.at[index])

    return copy


def stats_kernel(chunk, step, x_hbm, out_ref, x_ref, sems):
    total, lanes = x_ref.shape
    copy = chunk_copies(x_hbm, x_ref, sems, chunk)
    chunks = total // chunk
    for index in range(chunks):
        copy(index).start()

    def one(index, carry):
        top, acc = carry
        copy(index).wait()
        base = index * chunk

        def max_step(i, best):
            for s in range(step // LANE_ROWS):
                row = pl.multiple_of(base + i * step + s * LANE_ROWS, LANE_ROWS)
                best = jnp.maximum(best, x_ref[pl.ds(row, LANE_ROWS), :])
            return best

        new_top = lax.fori_loop(0, chunk // step, max_step, top)
        wide = new_top.astype(jnp.float32)
        acc = acc * jnp.exp2((top.astype(jnp.float32) - wide) * LOG2E)

        def sum_step(i, total_sum):
            for s in range(step // LANE_ROWS):
                row = pl.multiple_of(base + i * step + s * LANE_ROWS, LANE_ROWS)
                values = x_ref[pl.ds(row, LANE_ROWS), :].astype(jnp.float32)
                total_sum = total_sum + jnp.exp2((values - wide) * LOG2E)
            return total_sum

        acc = lax.fori_loop(0, chunk // step, sum_step, acc)
        return new_top, acc

    start = (
        jnp.full((LANE_ROWS, lanes), -3.0e38, jnp.bfloat16),
        jnp.zeros((LANE_ROWS, lanes), jnp.float32),
    )
    top, acc = lax.fori_loop(0, chunks, one, start)
    wide = top.astype(jnp.float32)
    row_top = jnp.max(wide, axis=0, keepdims=True)
    row_sum = jnp.sum(acc * jnp.exp2((wide - row_top) * LOG2E), axis=0, keepdims=True)
    out_ref[0:1, :] = row_top
    out_ref[1:2, :] = row_sum
    out_ref[2:, :] = jnp.zeros((out_ref.shape[0] - 2, lanes), jnp.float32)


def dense_rows(ids_ref, targets_ref, first_row, shape):
    row = lax.broadcasted_iota(jnp.int32, shape, 0) + first_row

    def add(j, dense):
        hit = ids_ref[pl.ds(j, 1), :] == row
        return dense + jnp.where(hit, targets_ref[pl.ds(j, 1), :], 0.0)

    return lax.fori_loop(0, ids_ref.shape[0], add, jnp.zeros(shape, jnp.float32))


def lists_kernel(
    blocks, bucket, group, place_ref, *refs
):
    routed = refs[:blocks]
    ids_ref, stats_ref, x_hbm = refs[blocks : blocks + 3]
    local_ref, targets_ref, index_ref, share_ref, value_ref, flag_ref, out_ref = refs[
        blocks + 3 : blocks + 10
    ]
    x_ref, over_ref, sems = refs[blocks + 10 :]
    total, lanes = x_ref.shape
    children = ids_ref.shape[0]
    buckets = total // bucket
    groups = buckets // group
    span = group * bucket
    slots = group * LANE_ROWS
    copy = chunk_copies(x_hbm, x_ref, sems, bucket)
    for index in range(buckets):
        copy(index).start()
    local = ids_ref[...] - place_ref[0]
    local_ref[...] = local

    position = lax.broadcasted_iota(jnp.int32, (lanes, lanes), 0) + place_ref[1]
    parts = jnp.zeros((3 * children, lanes), jnp.float32)
    for block in routed:
        owner = block[children : children + 1, :].astype(jnp.int32)
        matcher = jnp.where(owner == position, 1.0, 0.0).astype(jnp.bfloat16)
        rest = block[:children, :]
        pieces = []
        for _ in range(3):
            piece = rest.astype(jnp.bfloat16)
            pieces.append(piece)
            rest = rest - piece.astype(jnp.float32)
        stacked = jnp.concatenate(pieces, axis=0)
        parts = parts + lax.dot_general(
            stacked, matcher, (((1,), (1,)), ((), ())), preferred_element_type=jnp.float32
        )
    targets = parts[:children] + parts[children : 2 * children] + parts[2 * children :]
    targets_ref[...] = targets

    counts = []
    for g in range(groups):
        inside = (local >= g * span) & (local < (g + 1) * span)
        counts.append(
            jnp.max(jnp.sum(jnp.where(inside, 1.0, 0.0), axis=0, keepdims=True)).astype(jnp.int32)
        )

    big = jnp.int32(1 << 30)
    slot_row = lax.broadcasted_iota(jnp.int32, (slots, lanes), 0)
    slot_base = (slot_row // LANE_ROWS) * bucket + slot_row % LANE_ROWS
    for g in range(groups):

        def push(r, carry, g=g):
            last, index, share = carry
            here = local_ref[...]
            later = jnp.where((here > last) & (here < (g + 1) * span), here, big)
            found = jnp.min(later, axis=0, keepdims=True)
            amount = jnp.sum(
                jnp.where(here == found, targets_ref[...], 0.0), axis=0, keepdims=True
            )
            away = found - (g * span) - slot_base
            hit = (away >= 0) & (away < bucket) & ((away & (LANE_ROWS - 1)) == 0)
            at = (away // LANE_ROWS).astype(jnp.float32)
            new_index = [jnp.where(hit, at, index[0])]
            new_share = [jnp.where(hit, amount, share[0])]
            for k in range(1, DEPTH + 1):
                new_index.append(jnp.where(hit, index[k - 1], index[k]))
            for k in range(1, DEPTH):
                new_share.append(jnp.where(hit, share[k - 1], share[k]))
            return found, tuple(new_index), tuple(new_share)

        none = jnp.full((slots, lanes), -1.0, jnp.float32)
        zero = jnp.zeros((slots, lanes), jnp.float32)
        first = jnp.full((1, lanes), g * span - 1, jnp.int32)
        _, index, share = lax.fori_loop(
            0, counts[g], push, (first, (none,) * (DEPTH + 1), (zero,) * DEPTH)
        )
        for k in range(DEPTH):
            index_ref[k, g * slots : (g + 1) * slots, :] = index[k].astype(jnp.bfloat16)
            share_ref[k, g * slots : (g + 1) * slots, :] = share[k]
        over_ref[g] = jnp.max(index[DEPTH], axis=0, keepdims=True)
    for g in range(groups):
        flag_ref[g] = jnp.where(jnp.max(over_ref[g]) >= 0.0, 1, 0).astype(jnp.int32)

    out_ref[...] = stats_ref[...]

    def pick(b, picked):
        copy(b).wait()
        base = pl.multiple_of(b * bucket, LANE_ROWS)
        at = pl.ds(pl.multiple_of(b * LANE_ROWS, LANE_ROWS), LANE_ROWS)

        def fast():
            index = [index_ref[k, at, :] for k in range(DEPTH)]
            found = [jnp.zeros((LANE_ROWS, lanes), jnp.bfloat16)] * DEPTH
            for i in range(bucket // LANE_ROWS):
                values = x_ref[pl.ds(base + i * LANE_ROWS, LANE_ROWS), :]
                mark = jnp.bfloat16(i)
                found = [jnp.where(index[k] == mark, values, found[k]) for k in range(DEPTH)]
            extra = jnp.zeros((LANE_ROWS, lanes), jnp.float32)
            for k in range(DEPTH):
                value_ref[k, at, :] = found[k]
                extra = extra + share_ref[k, at, :] * found[k].astype(jnp.float32)
            return extra

        def slow():
            def add(i, extra):
                row = pl.multiple_of(base + i * LANE_ROWS, LANE_ROWS)
                dense = dense_rows(local_ref, targets_ref, row, (LANE_ROWS, lanes))
                values = x_ref[pl.ds(row, LANE_ROWS), :].astype(jnp.float32)
                return extra + jnp.where(dense != 0.0, dense * values, 0.0)

            zero = jnp.zeros((LANE_ROWS, lanes), jnp.float32)
            for k in range(DEPTH):
                value_ref[k, at, :] = zero.astype(jnp.bfloat16)
            return lax.fori_loop(0, bucket // LANE_ROWS, add, zero)

        return picked + lax.cond(flag_ref[b // group] == 0, fast, slow)

    picked = lax.fori_loop(0, buckets, pick, jnp.zeros((LANE_ROWS, lanes), jnp.float32))
    out_ref[2:3, :] = jnp.sum(picked, axis=0, keepdims=True)


def gradient_kernel(
    bucket,
    group,
    flag_ref,
    lse_ref,
    local_ref,
    targets_ref,
    index_ref,
    share_ref,
    value_ref,
    x_hbm,
    out_hbm,
    x_ref,
    out_ref,
    in_sems,
    out_sems,
):
    total, lanes = x_ref.shape
    buckets = total // bucket
    copy = chunk_copies(x_hbm, x_ref, in_sems, bucket)

    def back(index):
        window = pl.ds(index * bucket, bucket)
        return pltpu.make_async_copy(out_ref.at[window, :], out_hbm.at[window, :], out_sems.at[index])

    for index in range(buckets):
        copy(index).start()
    lse = jnp.broadcast_to(lse_ref[0:1, :], (LANE_ROWS, lanes))

    def one(b, carry):
        copy(b).wait()
        base = pl.multiple_of(b * bucket, LANE_ROWS)
        at = pl.ds(pl.multiple_of(b * LANE_ROWS, LANE_ROWS), LANE_ROWS)

        @pl.when(flag_ref[b // group] == 0)
        def _():
            index = [index_ref[k, at, :] for k in range(DEPTH)]
            given = []
            for k in range(DEPTH):
                value = value_ref[k, at, :].astype(jnp.float32)
                soft = jnp.exp2((value - lse) * LOG2E)
                given.append((soft - share_ref[k, at, :]).astype(jnp.bfloat16))
            for i in range(bucket // LANE_ROWS):
                row = pl.ds(base + i * LANE_ROWS, LANE_ROWS)
                values = x_ref[row, :].astype(jnp.float32)
                result = jnp.exp2((values - lse) * LOG2E).astype(jnp.bfloat16)
                mark = jnp.bfloat16(i)
                for k in range(DEPTH):
                    result = jnp.where(index[k] == mark, given[k], result)
                out_ref[row, :] = result

        @pl.when(flag_ref[b // group] != 0)
        def _():
            def fill(i, unused):
                first = pl.multiple_of(base + i * LANE_ROWS, LANE_ROWS)
                dense = dense_rows(local_ref, targets_ref, first, (LANE_ROWS, lanes))
                row = pl.ds(first, LANE_ROWS)
                values = x_ref[row, :].astype(jnp.float32)
                out_ref[row, :] = (jnp.exp2((values - lse) * LOG2E) - dense).astype(jnp.bfloat16)
                return unused

            lax.fori_loop(0, bucket // LANE_ROWS, fill, 0)

        back(b).start()
        return carry

    lax.fori_loop(0, buckets, one, 0)
    for index in range(buckets):
        back(index).wait()


def shifted(value, axis, size):
    result = []
    for shift in range(1, size):
        pairs = [(i, (i + shift) % size) for i in range(size)]
        result.append(lax.ppermute(value, axis, pairs))
    return result


def merge(one, other):
    top = jnp.maximum(one[0:1], other[0:1])
    total = one[1:2] * jnp.exp(one[0:1] - top) + other[1:2] * jnp.exp(other[0:1] - top)
    picked = one[2:3] + other[2:3]
    return jnp.concatenate([top, total, picked, jnp.zeros_like(one[3:])], axis=0)


def body(logits, child_ids, leaf_counts, leaf_valid, leaf_temp, leaf_owner):
    lanes, columns = logits.shape
    children = child_ids.shape[1]
    groups = lax.axis_size("dp")
    shards = lax.axis_size("tensor")
    f32 = jnp.float32
    params = pltpu.CompilerParams(vmem_limit_bytes=VMEM_BYTES)
    x = logits.T
    ids = child_ids.T
    place = jnp.stack([lax.axis_index("tensor") * columns, lax.axis_index("dp") * lanes])
    place = place.astype(jnp.int32)

    leaf = pl.pallas_call(
        prepare_kernel,
        out_shape=jax.ShapeDtypeStruct((children + 8, lanes), f32),
        name="prepare",
    )(
        leaf_counts.T,
        leaf_valid.reshape(1, lanes),
        leaf_temp.reshape(1, lanes),
        leaf_owner.reshape(1, lanes),
    )
    routed = [leaf] + shifted(leaf, "dp", groups)

    chunk = largest_block(columns, 2112)
    step = largest_block(chunk, 192)
    stats = pl.pallas_call(
        functools.partial(stats_kernel, chunk, step),
        out_shape=jax.ShapeDtypeStruct((8, lanes), f32),
        in_specs=[any_spec()],
        out_specs=vmem_spec(),
        scratch_shapes=[
            pltpu.VMEM((columns, lanes), jnp.bfloat16),
            pltpu.SemaphoreType.DMA((columns // chunk,)),
        ],
        compiler_params=params,
        name="stats",
    )(x)

    bucket = largest_block(columns, 704)
    buckets = columns // bucket
    group = 3 if buckets % 3 == 0 else 1
    listed = (DEPTH, buckets * LANE_ROWS, lanes)
    local, targets, index, share, value, flags, sums = pl.pallas_call(
        functools.partial(lists_kernel, groups, bucket, group),
        out_shape=(
            jax.ShapeDtypeStruct((children, lanes), jnp.int32),
            jax.ShapeDtypeStruct((children, lanes), f32),
            jax.ShapeDtypeStruct(listed, jnp.bfloat16),
            jax.ShapeDtypeStruct(listed, f32),
            jax.ShapeDtypeStruct(listed, jnp.bfloat16),
            jax.ShapeDtypeStruct((buckets // group,), jnp.int32),
            jax.ShapeDtypeStruct((8, lanes), f32),
        ),
        in_specs=[smem_spec()] + [vmem_spec()] * (groups + 2) + [any_spec()],
        out_specs=(vmem_spec(),) * 5 + (smem_spec(), vmem_spec()),
        scratch_shapes=[
            pltpu.VMEM((columns, lanes), jnp.bfloat16),
            pltpu.VMEM((buckets // group, 1, lanes), f32),
            pltpu.SemaphoreType.DMA((buckets,)),
        ],
        compiler_params=params,
        name="lists",
    )(place, *routed, ids, stats, x)

    hop = 1
    while hop < shards:
        pairs = [(i, i ^ hop) for i in range(shards)]
        sums = merge(sums, lax.ppermute(sums, "tensor", pairs))
        hop *= 2
    lse = sums[0:1] + jnp.log(sums[1:2])
    losses = lse - sums[2:3]
    row_loss = losses.reshape(lanes)
    own = jnp.broadcast_to(jnp.sum(losses), (8, 128))
    gathered = lax.all_gather(own[0:1, 0:1], "dp")
    mean_loss = jnp.sum(gathered) / (groups * lanes)

    gradient = pl.pallas_call(
        functools.partial(gradient_kernel, bucket, group),
        out_shape=jax.ShapeDtypeStruct((columns, lanes), jnp.bfloat16),
        in_specs=[smem_spec()] + [vmem_spec()] * 6 + [any_spec()],
        out_specs=any_spec(),
        scratch_shapes=[
            pltpu.VMEM((columns, lanes), jnp.bfloat16),
            pltpu.VMEM((columns, lanes), jnp.bfloat16),
            pltpu.SemaphoreType.DMA((buckets,)),
            pltpu.SemaphoreType.DMA((buckets,)),
        ],
        compiler_params=params,
        name="gradient",
    )(flags, lse, local, targets, index, share, value, x)
    return gradient.T, row_loss, mean_loss


def solution(mesh):
    return jax.shard_map(
        body,
        mesh=mesh,
        in_specs=(P("dp", "tensor"), P("dp", None), P("dp", None), P("dp"), P("dp"), P("dp")),
        out_specs=(P("dp", "tensor"), P("dp"), P()),
        check_vma=False,
    )
```

```python
import functools
import math

import jax
import jax.numpy as jnp
from jax import lax
from jax.experimental import pallas as pl
from jax.experimental.pallas import tpu as pltpu
from jax.sharding import PartitionSpec as P

LOG2E = 1.4426950408889634
LANE_ROWS = 16
DEPTH = 3
UNROLL = 4
VMEM_BYTES = 32 * 1024 * 1024


def largest_block(rows, limit):
    units = rows // LANE_ROWS
    best = 1
    for size in range(1, units + 1):
        if units % size == 0 and size * LANE_ROWS <= limit:
            best = size
    return best * LANE_ROWS


def any_spec():
    return pl.BlockSpec(memory_space=pltpu.HBM)


def vmem_spec():
    return pl.BlockSpec(memory_space=pltpu.VMEM)


def smem_spec():
    return pl.BlockSpec(memory_space=pltpu.SMEM)


def prepare_kernel(counts_ref, valid_ref, temp_ref, owner_ref, out_ref):
    children, rows = counts_ref.shape
    slot = lax.broadcasted_iota(jnp.int32, (children, rows), 0)
    powered = jnp.exp(jnp.log(counts_ref[...].astype(jnp.float32)) * temp_ref[...])
    weights = jnp.where(slot < valid_ref[...], powered, 0.0)
    out_ref[:children, :] = weights / jnp.sum(weights, axis=0, keepdims=True)
    extra = out_ref.shape[0] - children
    out_ref[children:, :] = jnp.broadcast_to(owner_ref[...].astype(jnp.float32), (extra, rows))


def stats_kernel(block, x_hbm, out_ref, x_ref, sems):
    total, lanes = x_ref.shape
    blocks = total // block
    units = block // LANE_ROWS

    def copy(index):
        window = pl.ds(index * block, block)
        return pltpu.make_async_copy(x_hbm.at[window, :], x_ref.at[window, :], sems.at[index])

    for index in range(blocks):
        copy(index).start()

    def block_top(index, best):
        base = pl.multiple_of(index * block, LANE_ROWS)
        for i in range(units):
            best = jnp.maximum(best, x_ref[pl.ds(base + i * LANE_ROWS, LANE_ROWS), :])
        return best

    def block_sum(index, wide, acc):
        base = pl.multiple_of(index * block, LANE_ROWS)
        for i in range(units):
            values = x_ref[pl.ds(base + i * LANE_ROWS, LANE_ROWS), :].astype(jnp.float32)
            acc = acc + jnp.exp2((values - wide) * LOG2E)
        return acc

    def one(index, carry):
        top, acc = carry
        copy(index + 1).wait()
        new_top = block_top(index + 1, top)
        wide = top.astype(jnp.float32)
        acc = block_sum(index, wide, acc)
        acc = acc * jnp.exp2((wide - new_top.astype(jnp.float32)) * LOG2E)
        return new_top, acc

    copy(0).wait()
    top = block_top(0, jnp.full((LANE_ROWS, lanes), -3.0e38, jnp.bfloat16))
    top, acc = lax.fori_loop(0, blocks - 1, one, (top, jnp.zeros((LANE_ROWS, lanes), jnp.float32)))
    wide = top.astype(jnp.float32)
    acc = block_sum(blocks - 1, wide, acc)
    row_top = jnp.max(wide, axis=0, keepdims=True)
    row_sum = jnp.sum(acc * jnp.exp2((wide - row_top) * LOG2E), axis=0, keepdims=True)
    out_ref[0:1, :] = row_top
    out_ref[1:2, :] = row_sum
    out_ref[2:, :] = jnp.zeros((out_ref.shape[0] - 2, lanes), jnp.float32)


def dense_rows(ids_ref, targets_ref, first_row, shape):
    row = lax.broadcasted_iota(jnp.int32, shape, 0) + first_row

    def add(j, dense):
        hit = ids_ref[pl.ds(j, 1), :] == row
        return dense + jnp.where(hit, targets_ref[pl.ds(j, 1), :], 0.0)

    return lax.fori_loop(0, ids_ref.shape[0], add, jnp.zeros(shape, jnp.float32))


def lists_kernel(leaf_blocks, bucket, group, *refs):
    routed = refs[:leaf_blocks]
    ids_ref, stats_ref, x_ref = refs[leaf_blocks : leaf_blocks + 3]
    local_ref, targets_ref, index_ref, share_ref, value_ref, flag_ref, out_ref = refs[
        leaf_blocks + 3 : leaf_blocks + 10
    ]
    code_ref, rank_ref, slot_ref, at_ref, part_ref = refs[leaf_blocks + 10 :]
    f32 = jnp.float32
    total, lanes = x_ref.shape
    children = ids_ref.shape[0]
    buckets = total // bucket
    groups = buckets // group
    units = bucket // LANE_ROWS
    slots = group * LANE_ROWS
    local = ids_ref[...] - lax.axis_index("tensor") * total
    local_ref[...] = local

    inside = (local >= 0) & (local < total)
    unit = local // LANE_ROWS
    at_bucket = ((unit.astype(f32) + 0.5) * (1.0 / units)).astype(jnp.int32)
    at = unit - at_bucket * units
    slot = at_bucket * LANE_ROWS + (local & (LANE_ROWS - 1))
    slot = jnp.where(inside, slot, -1)
    slot_ref[:children, :] = slot
    code_ref[...] = slot * 256 + at + 1

    tiles = children // 8
    sublane = lax.broadcasted_iota(jnp.int32, (8, lanes), 0)
    tile_slot = [slot[8 * t : 8 * t + 8] for t in range(tiles)]
    depth = [jnp.zeros((8, lanes), jnp.int32) for _ in range(tiles)]
    for j in range(children):
        row = slot_ref[j : j + 1, :]
        own = j // 8
        hit = (tile_slot[own] == row) & (sublane > j % 8)
        depth[own] = depth[own] + jnp.where(hit, 1, 0)
        for t in range(own + 1, tiles):
            depth[t] = depth[t] + jnp.where(tile_slot[t] == row, 1, 0)
    depth = jnp.where(inside, jnp.concatenate(depth, axis=0), -1)

    lower = lax.broadcasted_iota(jnp.int32, (children, children), 0)
    lower = lower > lax.broadcasted_iota(jnp.int32, (children, children), 1)
    lower = jnp.where(lower, 1.0, 0.0).astype(jnp.bfloat16)
    counts = []
    for k in range(DEPTH):
        chosen = jnp.where(depth == k, 1.0, 0.0)
        rank = jnp.dot(lower, chosen.astype(jnp.bfloat16), preferred_element_type=f32)
        rank_ref[k] = jnp.where(depth == k, rank, -1.0)
        counts.append(jnp.max(jnp.sum(chosen, axis=0, keepdims=True)).astype(jnp.int32))
    deepest = jnp.max(depth.astype(f32)).astype(jnp.int32)

    position = lax.broadcasted_iota(jnp.int32, (lanes, lanes), 0) + lax.axis_index("dp") * lanes
    parts = jnp.zeros((3 * children, lanes), f32)
    for block in routed:
        owner = block[children : children + 1, :].astype(jnp.int32)
        matcher = jnp.where(owner == position, 1.0, 0.0).astype(jnp.bfloat16)
        rest = block[:children, :]
        pieces = []
        for _ in range(3):
            piece = rest.astype(jnp.bfloat16)
            pieces.append(piece)
            rest = rest - piece.astype(f32)
        stacked = jnp.concatenate(pieces, axis=0)
        parts = parts + lax.dot_general(
            stacked, matcher, (((1,), (1,)), ((), ())), preferred_element_type=f32
        )
    targets_ref[...] = parts[:children] + parts[children : 2 * children] + parts[2 * children :]

    for g in range(groups):
        flag_ref[g] = 0

    @pl.when(deepest >= DEPTH)
    def _():
        for g in range(groups):
            over = (depth >= DEPTH) & (slot >= g * slots) & (slot < (g + 1) * slots)
            flag_ref[g] = jnp.max(jnp.where(over, 1.0, 0.0)).astype(jnp.int32)

    steps = [(count + UNROLL - 1) // UNROLL for count in counts]
    for k in range(DEPTH):

        def compact(step, unused, k=k):
            for u in range(UNROLL):
                r = step * UNROLL + u
                hit = rank_ref[k] == r.astype(f32)
                code = jnp.sum(jnp.where(hit, code_ref[...], 0), axis=0, keepdims=True) - 1
                part = jnp.sum(jnp.where(hit, targets_ref[...], 0.0), axis=0, keepdims=True)
                row = pl.ds(k * children + r, 1)
                slot_ref[row, :] = code >> 8
                at_ref[row, :] = (code & 255).astype(f32)
                part_ref[row, :] = part
            return unused

        lax.fori_loop(0, steps[k], compact, 0)

    def fill(g, unused):
        slot_row = lax.broadcasted_iota(jnp.int32, (slots, lanes), 0) + g * slots
        index, share = [], []
        for k in range(DEPTH):

            def add(step, carry, k=k):
                found, amount = carry
                for u in range(UNROLL):
                    row = pl.ds(k * children + step * UNROLL + u, 1)
                    hit = slot_ref[row, :] == slot_row
                    found = jnp.where(hit, at_ref[row, :], found)
                    amount = jnp.where(hit, part_ref[row, :], amount)
                return found, amount

            none = jnp.full((slots, lanes), -1.0, f32)
            zero = jnp.zeros((slots, lanes), f32)
            found, amount = lax.fori_loop(0, steps[k], add, (none, zero))
            for earlier in range(k):
                same = index[earlier] == found
                share[earlier] = share[earlier] + jnp.where(same, amount, 0.0)
                found = jnp.where(same, -1.0, found)
                amount = jnp.where(same, 0.0, amount)
            index.append(found)
            share.append(amount)
        rows = pl.ds(pl.multiple_of(g * slots, LANE_ROWS), slots)
        for k in range(DEPTH):
            index_ref[k, rows, :] = index[k].astype(jnp.bfloat16)
            share_ref[k, rows, :] = share[k]
        return unused

    lax.fori_loop(0, groups, fill, 0)
    out_ref[...] = stats_ref[...]

    def pick(b, picked):
        base = pl.multiple_of(b * bucket, LANE_ROWS)
        at_rows = pl.ds(pl.multiple_of(b * LANE_ROWS, LANE_ROWS), LANE_ROWS)

        def fast():
            index = [index_ref[k, at_rows, :] for k in range(DEPTH)]
            found = [jnp.zeros((LANE_ROWS, lanes), jnp.bfloat16)] * DEPTH
            for i in range(units):
                values = x_ref[pl.ds(base + i * LANE_ROWS, LANE_ROWS), :]
                mark = jnp.bfloat16(i)
                found = [jnp.where(index[k] == mark, values, found[k]) for k in range(DEPTH)]
            extra = jnp.zeros((LANE_ROWS, lanes), f32)
            for k in range(DEPTH):
                value_ref[k, at_rows, :] = found[k]
                extra = extra + share_ref[k, at_rows, :] * found[k].astype(f32)
            return extra

        def slow():
            def add(i, extra):
                row = pl.multiple_of(base + i * LANE_ROWS, LANE_ROWS)
                dense = dense_rows(local_ref, targets_ref, row, (LANE_ROWS, lanes))
                values = x_ref[pl.ds(row, LANE_ROWS), :].astype(f32)
                return extra + dense * values

            zero = jnp.zeros((LANE_ROWS, lanes), f32)
            for k in range(DEPTH):
                value_ref[k, at_rows, :] = zero.astype(jnp.bfloat16)
            return lax.fori_loop(0, units, add, zero)

        return picked + lax.cond(flag_ref[b // group] == 0, fast, slow)

    picked = lax.fori_loop(0, buckets, pick, jnp.zeros((LANE_ROWS, lanes), f32))
    out_ref[2:3, :] = jnp.sum(picked, axis=0, keepdims=True)


def gradient_kernel(
    bucket,
    group,
    flag_ref,
    lse_ref,
    own_ref,
    local_ref,
    targets_ref,
    index_ref,
    share_ref,
    value_ref,
    x_ref,
    out_hbm,
    loss_ref,
    out_ref,
    sems,
):
    total, lanes = x_ref.shape
    buckets = total // bucket

    def back(index):
        window = pl.ds(index * bucket, bucket)
        return pltpu.make_async_copy(out_ref.at[window, :], out_hbm.at[window, :], sems.at[index])

    loss_ref[...] = own_ref[...]
    lse = jnp.broadcast_to(lse_ref[0:1, :], (LANE_ROWS, lanes))

    def one(b, carry):
        base = pl.multiple_of(b * bucket, LANE_ROWS)
        at = pl.ds(pl.multiple_of(b * LANE_ROWS, LANE_ROWS), LANE_ROWS)

        @pl.when(flag_ref[b // group] == 0)
        def _():
            index = [index_ref[k, at, :] for k in range(DEPTH)]
            given = []
            for k in range(DEPTH):
                value = value_ref[k, at, :].astype(jnp.float32)
                soft = jnp.exp2((value - lse) * LOG2E)
                given.append((soft - share_ref[k, at, :]).astype(jnp.bfloat16))
            for i in range(bucket // LANE_ROWS):
                row = pl.ds(base + i * LANE_ROWS, LANE_ROWS)
                values = x_ref[row, :].astype(jnp.float32)
                result = jnp.exp2((values - lse) * LOG2E).astype(jnp.bfloat16)
                mark = jnp.bfloat16(i)
                for k in range(DEPTH):
                    result = jnp.where(index[k] == mark, given[k], result)
                out_ref[row, :] = result

        @pl.when(flag_ref[b // group] != 0)
        def _():
            def fill(i, unused):
                first = pl.multiple_of(base + i * LANE_ROWS, LANE_ROWS)
                dense = dense_rows(local_ref, targets_ref, first, (LANE_ROWS, lanes))
                row = pl.ds(first, LANE_ROWS)
                values = x_ref[row, :].astype(jnp.float32)
                out_ref[row, :] = (jnp.exp2((values - lse) * LOG2E) - dense).astype(jnp.bfloat16)
                return unused

            lax.fori_loop(0, bucket // LANE_ROWS, fill, 0)

        back(b).start()
        return carry

    lax.fori_loop(0, buckets, one, 0)
    for index in range(buckets):
        back(index).wait()


def shifted(value, axis, size):
    result = []
    for shift in range(1, size):
        pairs = [(i, i ^ shift) for i in range(size)]
        result.append(lax.ppermute(value, axis, pairs))
    return result


def merge(one, other):
    top = jnp.maximum(one[0:1], other[0:1])
    total = one[1:2] * jnp.exp(one[0:1] - top) + other[1:2] * jnp.exp(other[0:1] - top)
    picked = one[2:3] + other[2:3]
    return jnp.concatenate([top, total, picked, jnp.zeros_like(one[3:])], axis=0)


def body(logits, child_ids, leaf_counts, leaf_valid, leaf_temp, leaf_owner):
    lanes, columns = logits.shape
    children = child_ids.shape[1]
    groups = lax.axis_size("dp")
    shards = lax.axis_size("tensor")
    f32 = jnp.float32
    params = pltpu.CompilerParams(vmem_limit_bytes=VMEM_BYTES)
    ids = child_ids.T

    leaf = pl.pallas_call(
        prepare_kernel,
        out_shape=jax.ShapeDtypeStruct((children + 8, lanes), f32),
        name="prepare",
    )(
        leaf_counts.T,
        leaf_valid.reshape(1, lanes),
        leaf_temp.reshape(1, lanes),
        leaf_owner.reshape(1, lanes),
    )
    routed = [leaf] + shifted(leaf, "dp", groups)

    bucket = largest_block(columns, 704)
    buckets = columns // bucket
    group = 3 if buckets % 3 == 0 else 1
    stats, x = pl.pallas_call(
        functools.partial(stats_kernel, bucket),
        out_shape=(
            jax.ShapeDtypeStruct((8, lanes), f32),
            jax.ShapeDtypeStruct((columns, lanes), jnp.bfloat16),
        ),
        in_specs=[any_spec()],
        out_specs=(vmem_spec(), vmem_spec()),
        scratch_shapes=[pltpu.SemaphoreType.DMA((buckets,))],
        compiler_params=params,
        name="stats",
    )(pltpu.with_memory_space_constraint(logits.T, pltpu.HBM))

    listed = (DEPTH, buckets * LANE_ROWS, lanes)
    compact = DEPTH * children + 8
    local, targets, index, share, value, flags, sums = pl.pallas_call(
        functools.partial(lists_kernel, groups, bucket, group),
        out_shape=(
            jax.ShapeDtypeStruct((children, lanes), jnp.int32),
            jax.ShapeDtypeStruct((children, lanes), f32),
            jax.ShapeDtypeStruct(listed, jnp.bfloat16),
            jax.ShapeDtypeStruct(listed, f32),
            jax.ShapeDtypeStruct(listed, jnp.bfloat16),
            jax.ShapeDtypeStruct((buckets // group,), jnp.int32),
            jax.ShapeDtypeStruct((8, lanes), f32),
        ),
        in_specs=[vmem_spec()] * (groups + 3),
        out_specs=(vmem_spec(),) * 5 + (smem_spec(), vmem_spec()),
        scratch_shapes=[
            pltpu.VMEM((children, lanes), jnp.int32),
            pltpu.VMEM((DEPTH, children, lanes), f32),
            pltpu.VMEM((compact, lanes), jnp.int32),
            pltpu.VMEM((compact, lanes), f32),
            pltpu.VMEM((compact, lanes), f32),
        ],
        compiler_params=params,
        name="lists",
    )(*routed, ids, stats, x)

    hop = 1
    while hop < shards:
        pairs = [(i, i ^ hop) for i in range(shards)]
        sums = merge(sums, lax.ppermute(sums, "tensor", pairs))
        hop *= 2
    lse = sums[0:1] + jnp.log(sums[1:2])
    own = lse - sums[2:3]
    others = shifted(own, "dp", groups)

    gradient, row_loss = pl.pallas_call(
        functools.partial(gradient_kernel, bucket, group),
        out_shape=(
            jax.ShapeDtypeStruct((columns, lanes), jnp.bfloat16),
            jax.ShapeDtypeStruct((1, lanes), f32),
        ),
        in_specs=[smem_spec()] + [vmem_spec()] * 8,
        out_specs=(any_spec(), vmem_spec()),
        scratch_shapes=[
            pltpu.VMEM((columns, lanes), jnp.bfloat16),
            pltpu.SemaphoreType.DMA((buckets,)),
        ],
        compiler_params=params,
        name="gradient",
    )(flags, lse, own, local, targets, index, share, value, x)
    losses = [own] + others
    while len(losses) > 1:
        losses = [losses[i] + losses[i + 1] for i in range(0, len(losses), 2)]
    mean_loss = jnp.sum(losses[0]) / (groups * lanes)
    return gradient.T, row_loss.reshape(lanes), mean_loss


def solution(mesh):
    return jax.shard_map(
        body,
        mesh=mesh,
        in_specs=(P("dp", "tensor"), P("dp", None), P("dp", None), P("dp"), P("dp"), P("dp")),
        out_specs=(P("dp", "tensor"), P("dp"), P()),
        check_vma=False,
    )
```

```python
import functools
import math

import jax
import jax.numpy as jnp
from jax import lax
from jax.experimental import pallas as pl
from jax.experimental.pallas import tpu as pltpu
from jax.sharding import PartitionSpec as P

LOG2E = 1.4426950408889634
LANE_ROWS = 16
DEPTH = 3
UNROLL = 4
VMEM_BYTES = 13 * 1024 * 1024


def largest_block(rows, limit):
    units = rows // LANE_ROWS
    best = 1
    for size in range(1, units + 1):
        if units % size == 0 and size * LANE_ROWS <= limit:
            best = size
    return best * LANE_ROWS


def any_spec():
    return pl.BlockSpec(memory_space=pltpu.HBM)


def in_hbm(array):
    return pltpu.with_memory_space_constraint(array, pltpu.HBM)


def vmem_spec():
    return pl.BlockSpec(memory_space=pltpu.VMEM)


def smem_spec():
    return pl.BlockSpec(memory_space=pltpu.SMEM)


def prepare_kernel(counts_ref, valid_ref, temp_ref, owner_ref, out_ref):
    children, rows = counts_ref.shape
    slot = lax.broadcasted_iota(jnp.int32, (children, rows), 0)
    powered = jnp.exp(jnp.log(counts_ref[...].astype(jnp.float32)) * temp_ref[...])
    weights = jnp.where(slot < valid_ref[...], powered, 0.0)
    out_ref[:children, :] = weights / jnp.sum(weights, axis=0, keepdims=True)
    extra = out_ref.shape[0] - children
    out_ref[children:, :] = jnp.broadcast_to(owner_ref[...].astype(jnp.float32), (extra, rows))


def stats_kernel(block, x_hbm, out_ref, x_ref, power_ref, top_ref, sems):
    total, lanes = x_ref.shape
    blocks = total // block
    units = block // LANE_ROWS

    def copy(index):
        window = pl.ds(index * block, block)
        return pltpu.make_async_copy(x_hbm.at[window, :], x_ref.at[window, :], sems.at[index])

    for index in range(blocks):
        copy(index).start()

    def view(ref, index):
        return ref.at[pl.ds(pl.multiple_of(index * block, LANE_ROWS), block), :]

    def block_top(index, best):
        x = view(x_ref, index)
        for i in range(units):
            best = jnp.maximum(best, x[i * LANE_ROWS : (i + 1) * LANE_ROWS, :])
        return best

    def block_sum(index, wide, acc):
        x, powers = view(x_ref, index), view(power_ref, index)
        top_ref[pl.ds(pl.multiple_of(index * LANE_ROWS, LANE_ROWS), LANE_ROWS), :] = wide
        for i in range(units):
            row = slice(i * LANE_ROWS, (i + 1) * LANE_ROWS)
            power = jnp.exp2((x[row, :].astype(jnp.float32) - wide) * LOG2E)
            powers[row, :] = power
            acc = acc + power
        return acc

    def one(index, carry):
        top, acc = carry
        copy(index + 1).wait()
        new_top = block_top(index + 1, top)
        wide = top.astype(jnp.float32)
        acc = block_sum(index, wide, acc)
        acc = acc * jnp.exp2((wide - new_top.astype(jnp.float32)) * LOG2E)
        return new_top, acc

    copy(0).wait()
    top = block_top(0, jnp.full((LANE_ROWS, lanes), -3.0e38, jnp.bfloat16))
    top, acc = lax.fori_loop(0, blocks - 1, one, (top, jnp.zeros((LANE_ROWS, lanes), jnp.float32)))
    wide = top.astype(jnp.float32)
    acc = block_sum(blocks - 1, wide, acc)
    row_top = jnp.max(wide, axis=0, keepdims=True)
    row_sum = jnp.sum(acc * jnp.exp2((wide - row_top) * LOG2E), axis=0, keepdims=True)
    out_ref[0:1, :] = row_top
    out_ref[1:2, :] = row_sum
    out_ref[2:, :] = jnp.zeros((out_ref.shape[0] - 2, lanes), jnp.float32)


def dense_rows(ids_ref, targets_ref, first_row, shape):
    row = lax.broadcasted_iota(jnp.int32, shape, 0) + first_row

    def add(j, dense):
        hit = ids_ref[pl.ds(j, 1), :] == row
        return dense + jnp.where(hit, targets_ref[pl.ds(j, 1), :], 0.0)

    return lax.fori_loop(0, ids_ref.shape[0], add, jnp.zeros(shape, jnp.float32))


def lists_kernel(leaf_blocks, bucket, group, *refs):
    routed = refs[:leaf_blocks]
    ids_ref, stats_ref, x_ref, _, *results = refs[leaf_blocks:]
    local_ref, targets_ref, index_ref, share_ref, value_ref, flag_ref, out_ref = results[:7]
    code_ref, rank_ref, slot_ref, at_ref, part_ref = results[7:]
    f32 = jnp.float32
    total, lanes = x_ref.shape
    children = ids_ref.shape[0]
    buckets = total // bucket
    groups = buckets // group
    units = bucket // LANE_ROWS
    slots = group * LANE_ROWS
    local = ids_ref[...] - lax.axis_index("tensor") * total
    local_ref[...] = local

    inside = (local >= 0) & (local < total)
    unit = local // LANE_ROWS
    at_bucket = ((unit.astype(f32) + 0.5) * (1.0 / units)).astype(jnp.int32)
    at = unit - at_bucket * units
    slot = at_bucket * LANE_ROWS + (local & (LANE_ROWS - 1))
    slot = jnp.where(inside, slot, -1)
    slot_ref[:children, :] = slot
    code_ref[...] = slot * 256 + at + 1

    tiles = children // 8
    sublane = lax.broadcasted_iota(jnp.int32, (8, lanes), 0)
    tile_slot = [slot[8 * t : 8 * t + 8] for t in range(tiles)]
    depth = [jnp.zeros((8, lanes), jnp.int32) for _ in range(tiles)]
    for j in range(children):
        row = slot_ref[j : j + 1, :]
        own = j // 8
        hit = (tile_slot[own] == row) & (sublane > j % 8)
        depth[own] = depth[own] + jnp.where(hit, 1, 0)
        for t in range(own + 1, tiles):
            depth[t] = depth[t] + jnp.where(tile_slot[t] == row, 1, 0)
    depth = jnp.where(inside, jnp.concatenate(depth, axis=0), -1)

    lower = lax.broadcasted_iota(jnp.int32, (children, children), 0)
    lower = lower > lax.broadcasted_iota(jnp.int32, (children, children), 1)
    lower = jnp.where(lower, 1.0, 0.0).astype(jnp.bfloat16)
    counts = []
    for k in range(DEPTH):
        chosen = jnp.where(depth == k, 1.0, 0.0)
        rank = jnp.dot(lower, chosen.astype(jnp.bfloat16), preferred_element_type=f32)
        rank_ref[k] = jnp.where(depth == k, rank, -1.0)
        counts.append(jnp.max(jnp.sum(chosen, axis=0, keepdims=True)).astype(jnp.int32))
    deepest = jnp.max(depth.astype(f32)).astype(jnp.int32)

    position = lax.broadcasted_iota(jnp.int32, (lanes, lanes), 0) + lax.axis_index("dp") * lanes
    parts = jnp.zeros((3 * children, lanes), f32)
    for block in routed:
        owner = block[children : children + 1, :].astype(jnp.int32)
        matcher = jnp.where(owner == position, 1.0, 0.0).astype(jnp.bfloat16)
        rest = block[:children, :]
        pieces = []
        for _ in range(3):
            piece = rest.astype(jnp.bfloat16)
            pieces.append(piece)
            rest = rest - piece.astype(f32)
        stacked = jnp.concatenate(pieces, axis=0)
        parts = parts + lax.dot_general(
            stacked, matcher, (((1,), (1,)), ((), ())), preferred_element_type=f32
        )
    targets_ref[...] = parts[:children] + parts[children : 2 * children] + parts[2 * children :]

    for b in range(buckets):
        flag_ref[b] = 0

    @pl.when(deepest >= DEPTH)
    def _():
        for g in range(groups):
            over = (depth >= DEPTH) & (slot >= g * slots) & (slot < (g + 1) * slots)
            flag = jnp.max(jnp.where(over, 1.0, 0.0)).astype(jnp.int32)
            for b in range(g * group, (g + 1) * group):
                flag_ref[b] = flag

    steps = [(count + UNROLL - 1) // UNROLL for count in counts]
    for k in range(DEPTH):

        def compact(step, unused, k=k):
            for u in range(UNROLL):
                r = step * UNROLL + u
                hit = rank_ref[k] == r.astype(f32)
                code = jnp.sum(jnp.where(hit, code_ref[...], 0), axis=0, keepdims=True) - 1
                part = jnp.sum(jnp.where(hit, targets_ref[...], 0.0), axis=0, keepdims=True)
                row = pl.ds(k * children + r, 1)
                slot_ref[row, :] = code >> 8
                at_ref[row, :] = (code & 255).astype(f32)
                part_ref[row, :] = part
            return unused

        lax.fori_loop(0, steps[k], compact, 0)

    def fill(g, unused):
        slot_row = lax.broadcasted_iota(jnp.int32, (slots, lanes), 0) + g * slots
        index, share = [], []
        for k in range(DEPTH):

            def add(step, carry, k=k):
                found, amount = carry
                for u in range(UNROLL):
                    row = pl.ds(k * children + step * UNROLL + u, 1)
                    hit = slot_ref[row, :] == slot_row
                    found = jnp.where(hit, at_ref[row, :], found)
                    amount = jnp.where(hit, part_ref[row, :], amount)
                return found, amount

            none = jnp.full((slots, lanes), -1.0, f32)
            zero = jnp.zeros((slots, lanes), f32)
            found, amount = lax.fori_loop(0, steps[k], add, (none, zero))
            for earlier in range(k):
                same = index[earlier] == found
                share[earlier] = share[earlier] + jnp.where(same, amount, 0.0)
                found = jnp.where(same, -1.0, found)
                amount = jnp.where(same, 0.0, amount)
            index.append(found)
            share.append(amount)
        rows = pl.ds(pl.multiple_of(g * slots, LANE_ROWS), slots)
        for k in range(DEPTH):
            index_ref[k, rows, :] = index[k].astype(jnp.bfloat16)
            share_ref[k, rows, :] = share[k]
        return unused

    lax.fori_loop(0, groups, fill, 0)
    out_ref[...] = stats_ref[...]

    def pick(b, picked):
        base = pl.multiple_of(b * bucket, LANE_ROWS)
        at_rows = pl.ds(pl.multiple_of(b * LANE_ROWS, LANE_ROWS), LANE_ROWS)

        def fast():
            index = [index_ref[k, at_rows, :] for k in range(DEPTH)]
            found = [jnp.zeros((LANE_ROWS, lanes), jnp.bfloat16)] * DEPTH
            x = x_ref.at[pl.ds(base, bucket), :]
            for i in range(units):
                values = x[i * LANE_ROWS : (i + 1) * LANE_ROWS, :]
                mark = jnp.bfloat16(i)
                found = [jnp.where(index[k] == mark, values, found[k]) for k in range(DEPTH)]
            extra = jnp.zeros((LANE_ROWS, lanes), f32)
            for k in range(DEPTH):
                value_ref[k, at_rows, :] = found[k]
                extra = extra + share_ref[k, at_rows, :] * found[k].astype(f32)
            return extra

        def slow():
            def add(i, extra):
                row = pl.multiple_of(base + i * LANE_ROWS, LANE_ROWS)
                dense = dense_rows(local_ref, targets_ref, row, (LANE_ROWS, lanes))
                values = x_ref[pl.ds(row, LANE_ROWS), :].astype(f32)
                return extra + dense * values

            zero = jnp.zeros((LANE_ROWS, lanes), f32)
            for k in range(DEPTH):
                value_ref[k, at_rows, :] = zero.astype(jnp.bfloat16)
            return lax.fori_loop(0, units, add, zero)

        return picked + lax.cond(flag_ref[b] == 0, fast, slow)

    picked = lax.fori_loop(0, buckets, pick, jnp.zeros((LANE_ROWS, lanes), f32))
    out_ref[2:3, :] = jnp.sum(picked, axis=0, keepdims=True)


def gradient_kernel(
    bucket,
    flag_ref,
    lse_ref,
    own_ref,
    local_ref,
    targets_ref,
    index_ref,
    share_ref,
    value_ref,
    power_ref,
    top_ref,
    out_hbm,
    loss_hbm,
    out_ref,
    sems,
    loss_sem,
):
    total, lanes = power_ref.shape
    buckets = total // bucket

    def back(index):
        window = pl.ds(index * bucket, bucket)
        return pltpu.make_async_copy(out_ref.at[window, :], out_hbm.at[window, :], sems.at[index])

    losses = pltpu.make_async_copy(own_ref, loss_hbm, loss_sem)
    losses.start()
    lse = jnp.broadcast_to(lse_ref[0:1, :], (LANE_ROWS, lanes))

    def one(b, carry):
        base = pl.multiple_of(b * bucket, LANE_ROWS)
        at = pl.ds(pl.multiple_of(b * LANE_ROWS, LANE_ROWS), LANE_ROWS)
        scale = jnp.exp2((top_ref[at, :] - lse) * LOG2E)

        @pl.when(flag_ref[b] == 0)
        def _():
            index = [index_ref[k, at, :] for k in range(DEPTH)]
            given = []
            for k in range(DEPTH):
                value = value_ref[k, at, :].astype(jnp.float32)
                soft = jnp.exp2((value - lse) * LOG2E)
                given.append((soft - share_ref[k, at, :]).astype(jnp.bfloat16))
            powers = power_ref.at[pl.ds(base, bucket), :]
            results = out_ref.at[pl.ds(base, bucket), :]
            for i in range(bucket // LANE_ROWS):
                row = slice(i * LANE_ROWS, (i + 1) * LANE_ROWS)
                result = (powers[row, :] * scale).astype(jnp.bfloat16)
                mark = jnp.bfloat16(i)
                for k in range(DEPTH):
                    result = jnp.where(index[k] == mark, given[k], result)
                results[row, :] = result

        @pl.when(flag_ref[b] != 0)
        def _():
            def fill(i, unused):
                first = pl.multiple_of(base + i * LANE_ROWS, LANE_ROWS)
                dense = dense_rows(local_ref, targets_ref, first, (LANE_ROWS, lanes))
                row = pl.ds(first, LANE_ROWS)
                out_ref[row, :] = (power_ref[row, :] * scale - dense).astype(jnp.bfloat16)
                return unused

            lax.fori_loop(0, bucket // LANE_ROWS, fill, 0)

        back(b).start()
        return carry

    lax.fori_loop(0, buckets, one, 0)
    for index in range(buckets):
        back(index).wait()
    losses.wait()


def shifted(value, axis, size):
    result = []
    for shift in range(1, size):
        pairs = [(i, i ^ shift) for i in range(size)]
        result.append(lax.ppermute(value, axis, pairs))
    return result


def merge(one, other):
    top = jnp.maximum(one[0:1], other[0:1])
    total = one[1:2] * jnp.exp(one[0:1] - top) + other[1:2] * jnp.exp(other[0:1] - top)
    picked = one[2:3] + other[2:3]
    return jnp.concatenate([top, total, picked, jnp.zeros_like(one[3:])], axis=0)


def body(logits, child_ids, leaf_counts, leaf_valid, leaf_temp, leaf_owner):
    lanes, columns = logits.shape
    children = child_ids.shape[1]
    groups = lax.axis_size("dp")
    shards = lax.axis_size("tensor")
    f32 = jnp.float32
    params = pltpu.CompilerParams(vmem_limit_bytes=VMEM_BYTES)
    ids = child_ids.T

    leaf = pl.pallas_call(
        prepare_kernel,
        out_shape=jax.ShapeDtypeStruct((children + 8, lanes), f32),
        compiler_params=params,
        name="prepare",
    )(
        in_hbm(leaf_counts.T),
        in_hbm(leaf_valid.reshape(1, lanes)),
        in_hbm(leaf_temp.reshape(1, lanes)),
        in_hbm(leaf_owner.reshape(1, lanes)),
    )
    routed = [leaf] + shifted(leaf, "dp", groups)

    bucket = largest_block(columns, 704)
    buckets = columns // bucket
    group = 3 if buckets % 3 == 0 else 1
    stats, x, power, tops = pl.pallas_call(
        functools.partial(stats_kernel, bucket),
        out_shape=(
            jax.ShapeDtypeStruct((8, lanes), f32),
            jax.ShapeDtypeStruct((columns, lanes), jnp.bfloat16),
            jax.ShapeDtypeStruct((columns, lanes), f32),
            jax.ShapeDtypeStruct((buckets * LANE_ROWS, lanes), f32),
        ),
        in_specs=[any_spec()],
        out_specs=(vmem_spec(),) * 4,
        scratch_shapes=[pltpu.SemaphoreType.DMA((buckets,))],
        compiler_params=params,
        name="stats",
    )(in_hbm(logits.T))

    listed = (DEPTH, buckets * LANE_ROWS, lanes)
    compact = DEPTH * children + 8
    local, targets, index, share, value, flags, sums = pl.pallas_call(
        functools.partial(lists_kernel, groups, bucket, group),
        out_shape=(
            jax.ShapeDtypeStruct((children, lanes), jnp.int32),
            jax.ShapeDtypeStruct((children, lanes), f32),
            jax.ShapeDtypeStruct(listed, jnp.bfloat16),
            jax.ShapeDtypeStruct(listed, f32),
            jax.ShapeDtypeStruct(listed, jnp.bfloat16),
            jax.ShapeDtypeStruct((buckets,), jnp.int32),
            jax.ShapeDtypeStruct((8, lanes), f32),
        ),
        in_specs=[vmem_spec()] * (groups + 4),
        out_specs=(vmem_spec(),) * 5 + (smem_spec(), vmem_spec()),
        scratch_shapes=[
            pltpu.VMEM((children, lanes), jnp.int32),
            pltpu.VMEM((DEPTH, children, lanes), f32),
            pltpu.VMEM((compact, lanes), jnp.int32),
            pltpu.VMEM((compact, lanes), f32),
            pltpu.VMEM((compact, lanes), f32),
        ],
        compiler_params=params,
        name="lists",
    )(*routed, ids, stats, x, power)

    hop = 1
    while hop < shards:
        pairs = [(i, i ^ hop) for i in range(shards)]
        sums = merge(sums, lax.ppermute(sums, "tensor", pairs))
        hop *= 2
    lse = sums[0:1] + jnp.log(sums[1:2])
    own = lse - sums[2:3]
    others = shifted(own, "dp", groups)

    gradient, row_loss = pl.pallas_call(
        functools.partial(gradient_kernel, bucket),
        out_shape=(
            jax.ShapeDtypeStruct((columns, lanes), jnp.bfloat16),
            jax.ShapeDtypeStruct((1, lanes), f32),
        ),
        in_specs=[smem_spec()] + [vmem_spec()] * 9,
        out_specs=(any_spec(), any_spec()),
        scratch_shapes=[
            pltpu.VMEM((columns, lanes), jnp.bfloat16),
            pltpu.SemaphoreType.DMA((buckets,)),
            pltpu.SemaphoreType.DMA(()),
        ],
        compiler_params=params,
        name="gradient",
    )(flags, lse, own, local, targets, index, share, value, power, tops)
    losses = [own] + others
    while len(losses) > 1:
        losses = [losses[i] + losses[i + 1] for i in range(0, len(losses), 2)]
    mean_loss = jnp.sum(losses[0]) / (groups * lanes)
    return gradient.T, row_loss.reshape(lanes), mean_loss


def solution(mesh):
    return jax.shard_map(
        body,
        mesh=mesh,
        in_specs=(P("dp", "tensor"), P("dp", None), P("dp", None), P("dp"), P("dp"), P("dp")),
        out_specs=(P("dp", "tensor"), P("dp"), P()),
        check_vma=False,
    )
```

```python
import functools
import math

import jax
import jax.numpy as jnp
from jax import lax
from jax.experimental import pallas as pl
from jax.experimental.pallas import tpu as pltpu
from jax.sharding import PartitionSpec as P

LOG2E = 1.4426950408889634
LANE_ROWS = 16
DEPTH = 3
UNROLL = 4
CHAINS = 4
USUAL = 2
VMEM_BYTES = 13 * 1024 * 1024


def largest_block(rows, limit):
    units = rows // LANE_ROWS
    best = 1
    for size in range(1, units + 1):
        if units % size == 0 and size * LANE_ROWS <= limit:
            best = size
    return best * LANE_ROWS


def any_spec():
    return pl.BlockSpec(memory_space=pltpu.HBM)


def in_hbm(array):
    return pltpu.with_memory_space_constraint(array, pltpu.HBM)


def vmem_spec():
    return pl.BlockSpec(memory_space=pltpu.VMEM)


def smem_spec():
    return pl.BlockSpec(memory_space=pltpu.SMEM)


def prepare_kernel(counts_ref, valid_ref, temp_ref, owner_ref, out_ref):
    children, rows = counts_ref.shape
    slot = lax.broadcasted_iota(jnp.int32, (children, rows), 0)
    powered = jnp.exp(jnp.log(counts_ref[...].astype(jnp.float32)) * temp_ref[...])
    weights = jnp.where(slot < valid_ref[...], powered, 0.0)
    out_ref[:children, :] = weights / jnp.sum(weights, axis=0, keepdims=True)
    extra = out_ref.shape[0] - children
    out_ref[children:, :] = jnp.broadcast_to(owner_ref[...].astype(jnp.float32), (extra, rows))


def stats_kernel(block, x_hbm, out_ref, x_ref, power_ref, top_ref, sems):
    total, lanes = x_ref.shape
    blocks = total // block
    units = block // LANE_ROWS

    def copy(index):
        window = pl.ds(index * block, block)
        return pltpu.make_async_copy(x_hbm.at[window, :], x_ref.at[window, :], sems.at[index])

    for index in range(blocks):
        copy(index).start()

    def view(ref, index):
        return ref.at[pl.ds(pl.multiple_of(index * block, LANE_ROWS), block), :]

    def block_pass(index, wide, acc, following, best):
        top_ref[pl.ds(pl.multiple_of(index * LANE_ROWS, LANE_ROWS), LANE_ROWS), :] = wide
        x, powers = view(x_ref, index), view(power_ref, index)
        following = None if following is None else view(x_ref, following)
        tops = [best] * CHAINS
        for i in range(units):
            row = slice(i * LANE_ROWS, (i + 1) * LANE_ROWS)
            power = jnp.exp2((x[row, :].astype(jnp.float32) - wide) * LOG2E)
            powers[row, :] = power
            acc = acc + power
            if following is not None:
                tops[i % CHAINS] = jnp.maximum(tops[i % CHAINS], following[row, :])
        return acc, functools.reduce(jnp.maximum, tops)

    def one(index, carry):
        top, acc = carry
        copy(index + 1).wait()
        wide = top.astype(jnp.float32)
        acc, new_top = block_pass(index, wide, acc, index + 1, top)
        acc = acc * jnp.exp2((wide - new_top.astype(jnp.float32)) * LOG2E)
        return new_top, acc

    copy(0).wait()
    first = view(x_ref, 0)
    tops = [first[i * LANE_ROWS : (i + 1) * LANE_ROWS, :] for i in range(units)]
    top = functools.reduce(jnp.maximum, tops)
    top, acc = lax.fori_loop(0, blocks - 1, one, (top, jnp.zeros((LANE_ROWS, lanes), jnp.float32)))
    wide = top.astype(jnp.float32)
    acc, _ = block_pass(blocks - 1, wide, acc, None, top)
    row_top = jnp.max(wide, axis=0, keepdims=True)
    row_sum = jnp.sum(acc * jnp.exp2((wide - row_top) * LOG2E), axis=0, keepdims=True)
    out_ref[0:1, :] = row_top
    out_ref[1:2, :] = row_sum
    out_ref[2:, :] = jnp.zeros((out_ref.shape[0] - 2, lanes), jnp.float32)


def dense_rows(ids_ref, targets_ref, first_row, shape):
    row = lax.broadcasted_iota(jnp.int32, shape, 0) + first_row

    def add(j, dense):
        hit = ids_ref[pl.ds(j, 1), :] == row
        return dense + jnp.where(hit, targets_ref[pl.ds(j, 1), :], 0.0)

    return lax.fori_loop(0, ids_ref.shape[0], add, jnp.zeros(shape, jnp.float32))


def lists_kernel(leaf_blocks, bucket, group, *refs):
    routed = refs[:leaf_blocks]
    ids_ref, stats_ref, x_ref, _, *results = refs[leaf_blocks:]
    local_ref, targets_ref, index_ref, share_ref, value_ref, flag_ref, out_ref = results[:7]
    code_ref, rank_ref, slot_ref, at_ref, part_ref = results[7:]
    f32 = jnp.float32
    total, lanes = x_ref.shape
    children = ids_ref.shape[0]
    buckets = total // bucket
    groups = buckets // group
    units = bucket // LANE_ROWS
    slots = group * LANE_ROWS
    local = ids_ref[...] - lax.axis_index("tensor") * total
    local_ref[...] = local

    inside = (local >= 0) & (local < total)
    unit = local // LANE_ROWS
    at_bucket = ((unit.astype(f32) + 0.5) * (1.0 / units)).astype(jnp.int32)
    at = unit - at_bucket * units
    slot = at_bucket * LANE_ROWS + (local & (LANE_ROWS - 1))
    slot = jnp.where(inside, slot, -1)
    slot_ref[:children, :] = slot
    code_ref[...] = slot * 256 + at + 1

    tiles = children // 8
    sublane = lax.broadcasted_iota(jnp.int32, (8, lanes), 0)
    tile_slot = [slot[8 * t : 8 * t + 8] for t in range(tiles)]
    depth = [jnp.zeros((8, lanes), jnp.int32) for _ in range(tiles)]
    for j in range(children):
        row = slot_ref[j : j + 1, :]
        own = j // 8
        hit = (tile_slot[own] == row) & (sublane > j % 8)
        depth[own] = depth[own] + jnp.where(hit, 1, 0)
        for t in range(own + 1, tiles):
            depth[t] = depth[t] + jnp.where(tile_slot[t] == row, 1, 0)
    depth = jnp.where(inside, jnp.concatenate(depth, axis=0), -1)

    lower = lax.broadcasted_iota(jnp.int32, (children, children), 0)
    lower = lower > lax.broadcasted_iota(jnp.int32, (children, children), 1)
    lower = jnp.where(lower, 1.0, 0.0).astype(jnp.bfloat16)
    counts = []
    for k in range(DEPTH):
        chosen = jnp.where(depth == k, 1.0, 0.0)
        rank = jnp.dot(lower, chosen.astype(jnp.bfloat16), preferred_element_type=f32)
        rank_ref[k] = jnp.where(depth == k, rank, -1.0)
        counts.append(jnp.max(jnp.sum(chosen, axis=0, keepdims=True)).astype(jnp.int32))
    deepest = jnp.max(depth.astype(f32)).astype(jnp.int32)

    position = lax.broadcasted_iota(jnp.int32, (lanes, lanes), 0) + lax.axis_index("dp") * lanes
    parts = jnp.zeros((3 * children, lanes), f32)
    for block in routed:
        owner = block[children : children + 1, :].astype(jnp.int32)
        matcher = jnp.where(owner == position, 1.0, 0.0).astype(jnp.bfloat16)
        rest = block[:children, :]
        pieces = []
        for _ in range(3):
            piece = rest.astype(jnp.bfloat16)
            pieces.append(piece)
            rest = rest - piece.astype(f32)
        stacked = jnp.concatenate(pieces, axis=0)
        parts = parts + lax.dot_general(
            stacked, matcher, (((1,), (1,)), ((), ())), preferred_element_type=f32
        )
    targets_ref[...] = parts[:children] + parts[children : 2 * children] + parts[2 * children :]

    third = jnp.where(depth >= USUAL, at_bucket.astype(f32), -1.0)
    last = jnp.max(third).astype(jnp.int32)
    third = jnp.where(depth >= USUAL, at_bucket.astype(f32), 1.0 * buckets)
    first = jnp.min(third).astype(jnp.int32)
    for b in range(buckets):
        flag_ref[b] = jnp.where((first <= b) & (last >= b), 1, 0).astype(jnp.int32)

    @pl.when(deepest >= DEPTH)
    def _():
        for g in range(groups):
            over = (depth >= DEPTH) & (slot >= g * slots) & (slot < (g + 1) * slots)
            flag = jnp.max(jnp.where(over, 1.0, 0.0)).astype(jnp.int32)
            for b in range(g * group, (g + 1) * group):
                flag_ref[b] = jnp.where(flag > 0, 2, flag_ref[b])

    steps = [(count + UNROLL - 1) // UNROLL for count in counts]
    for k in range(DEPTH):

        def compact(step, unused, k=k):
            for u in range(UNROLL):
                r = step * UNROLL + u
                hit = rank_ref[k] == r.astype(f32)
                code = jnp.sum(jnp.where(hit, code_ref[...], 0), axis=0, keepdims=True) - 1
                part = jnp.sum(jnp.where(hit, targets_ref[...], 0.0), axis=0, keepdims=True)
                row = pl.ds(k * children + r, 1)
                slot_ref[row, :] = code >> 8
                at_ref[row, :] = (code & 255).astype(f32)
                part_ref[row, :] = part
            return unused

        lax.fori_loop(0, steps[k], compact, 0)

    def fill(g, unused, levels):
        slot_row = lax.broadcasted_iota(jnp.int32, (slots, lanes), 0) + g * slots
        rows = pl.ds(pl.multiple_of(g * slots, LANE_ROWS), slots)
        index = [index_ref[k, rows, :].astype(f32) for k in range(levels[0])]
        share = [share_ref[k, rows, :] for k in range(levels[0])]
        for k in levels:

            def add(step, carry, k=k):
                found, amount = carry
                for u in range(UNROLL):
                    row = pl.ds(k * children + step * UNROLL + u, 1)
                    hit = slot_ref[row, :] == slot_row
                    found = jnp.where(hit, at_ref[row, :], found)
                    amount = jnp.where(hit, part_ref[row, :], amount)
                return found, amount

            none = jnp.full((slots, lanes), -1.0, f32)
            zero = jnp.zeros((slots, lanes), f32)
            found, amount = lax.fori_loop(0, steps[k], add, (none, zero))
            for earlier in range(k):
                same = index[earlier] == found
                share[earlier] = share[earlier] + jnp.where(same, amount, 0.0)
                found = jnp.where(same, -1.0, found)
                amount = jnp.where(same, 0.0, amount)
            index.append(found)
            share.append(amount)
        for k in range(levels[-1] + 1):
            if k in levels:
                index_ref[k, rows, :] = index[k].astype(jnp.bfloat16)
            share_ref[k, rows, :] = share[k]
        return unused

    lax.fori_loop(0, groups, functools.partial(fill, levels=tuple(range(USUAL))), 0)

    @pl.when(deepest >= USUAL)
    def _():
        lax.fori_loop(0, groups, functools.partial(fill, levels=tuple(range(USUAL, DEPTH))), 0)

    out_ref[...] = stats_ref[...]

    def pick(b, picked):
        base = pl.multiple_of(b * bucket, LANE_ROWS)
        at_rows = pl.ds(pl.multiple_of(b * LANE_ROWS, LANE_ROWS), LANE_ROWS)

        def fast(entries):
            index = [index_ref[k, at_rows, :] for k in range(entries)]
            found = [jnp.zeros((LANE_ROWS, lanes), jnp.bfloat16)] * entries
            x = x_ref.at[pl.ds(base, bucket), :]
            for i in range(units):
                values = x[i * LANE_ROWS : (i + 1) * LANE_ROWS, :]
                mark = jnp.bfloat16(i)
                found = [jnp.where(index[k] == mark, values, found[k]) for k in range(entries)]
            extra = jnp.zeros((LANE_ROWS, lanes), f32)
            for k in range(entries):
                value_ref[k, at_rows, :] = found[k]
                extra = extra + share_ref[k, at_rows, :] * found[k].astype(f32)
            return extra

        def slow():
            def add(i, extra):
                row = pl.multiple_of(base + i * LANE_ROWS, LANE_ROWS)
                dense = dense_rows(local_ref, targets_ref, row, (LANE_ROWS, lanes))
                values = x_ref[pl.ds(row, LANE_ROWS), :].astype(f32)
                return extra + dense * values

            zero = jnp.zeros((LANE_ROWS, lanes), f32)
            for k in range(DEPTH):
                value_ref[k, at_rows, :] = zero.astype(jnp.bfloat16)
            return lax.fori_loop(0, units, add, zero)

        usual = functools.partial(fast, USUAL)
        deeper = functools.partial(fast, DEPTH)
        rare = lambda: lax.cond(flag_ref[b] == 1, deeper, slow)
        return picked + lax.cond(flag_ref[b] == 0, usual, rare)

    picked = lax.fori_loop(0, buckets, pick, jnp.zeros((LANE_ROWS, lanes), f32))
    out_ref[2:3, :] = jnp.sum(picked, axis=0, keepdims=True)


def gradient_kernel(
    bucket,
    flag_ref,
    lse_ref,
    own_ref,
    local_ref,
    targets_ref,
    index_ref,
    share_ref,
    value_ref,
    power_ref,
    top_ref,
    out_hbm,
    loss_hbm,
    out_ref,
    sems,
    loss_sem,
):
    total, lanes = power_ref.shape
    buckets = total // bucket

    def back(index):
        window = pl.ds(index * bucket, bucket)
        return pltpu.make_async_copy(out_ref.at[window, :], out_hbm.at[window, :], sems.at[index])

    losses = pltpu.make_async_copy(own_ref, loss_hbm, loss_sem)
    losses.start()
    lse = jnp.broadcast_to(lse_ref[0:1, :], (LANE_ROWS, lanes))

    def one(b, carry):
        base = pl.multiple_of(b * bucket, LANE_ROWS)
        at = pl.ds(pl.multiple_of(b * LANE_ROWS, LANE_ROWS), LANE_ROWS)
        scale = jnp.exp2((top_ref[at, :] - lse) * LOG2E)

        def listed(entries):
            index = [index_ref[k, at, :] for k in range(entries)]
            given = []
            for k in range(entries):
                value = value_ref[k, at, :].astype(jnp.float32)
                soft = jnp.exp2((value - lse) * LOG2E)
                given.append((soft - share_ref[k, at, :]).astype(jnp.bfloat16))
            powers = power_ref.at[pl.ds(base, bucket), :]
            results = out_ref.at[pl.ds(base, bucket), :]
            for i in range(bucket // LANE_ROWS):
                row = slice(i * LANE_ROWS, (i + 1) * LANE_ROWS)
                result = (powers[row, :] * scale).astype(jnp.bfloat16)
                mark = jnp.bfloat16(i)
                for k in range(entries):
                    result = jnp.where(index[k] == mark, given[k], result)
                results[row, :] = result

        pl.when(flag_ref[b] == 0)(functools.partial(listed, USUAL))
        pl.when(flag_ref[b] == 1)(functools.partial(listed, DEPTH))

        @pl.when(flag_ref[b] == 2)
        def _():
            def fill(i, unused):
                first = pl.multiple_of(base + i * LANE_ROWS, LANE_ROWS)
                dense = dense_rows(local_ref, targets_ref, first, (LANE_ROWS, lanes))
                row = pl.ds(first, LANE_ROWS)
                out_ref[row, :] = (power_ref[row, :] * scale - dense).astype(jnp.bfloat16)
                return unused

            lax.fori_loop(0, bucket // LANE_ROWS, fill, 0)

        back(b).start()
        return carry

    lax.fori_loop(0, buckets, one, 0)
    for index in range(buckets):
        back(index).wait()
    losses.wait()


def shifted(value, axis, size):
    result = []
    for shift in range(1, size):
        pairs = [(i, i ^ shift) for i in range(size)]
        result.append(lax.ppermute(value, axis, pairs))
    return result


def merge(one, other):
    top = jnp.maximum(one[0:1], other[0:1])
    total = one[1:2] * jnp.exp(one[0:1] - top) + other[1:2] * jnp.exp(other[0:1] - top)
    picked = one[2:3] + other[2:3]
    return jnp.concatenate([top, total, picked, jnp.zeros_like(one[3:])], axis=0)


def body(logits, child_ids, leaf_counts, leaf_valid, leaf_temp, leaf_owner):
    lanes, columns = logits.shape
    children = child_ids.shape[1]
    groups = lax.axis_size("dp")
    shards = lax.axis_size("tensor")
    f32 = jnp.float32
    params = pltpu.CompilerParams(vmem_limit_bytes=VMEM_BYTES)
    ids = child_ids.T

    leaf = pl.pallas_call(
        prepare_kernel,
        out_shape=jax.ShapeDtypeStruct((children + 8, lanes), f32),
        compiler_params=params,
        name="prepare",
    )(
        in_hbm(leaf_counts.T),
        in_hbm(leaf_valid.reshape(1, lanes)),
        in_hbm(leaf_temp.reshape(1, lanes)),
        in_hbm(leaf_owner.reshape(1, lanes)),
    )
    routed = [leaf] + shifted(leaf, "dp", groups)

    bucket = largest_block(columns, 704)
    buckets = columns // bucket
    group = 3 if buckets % 3 == 0 else 1
    stats, x, power, tops = pl.pallas_call(
        functools.partial(stats_kernel, bucket),
        out_shape=(
            jax.ShapeDtypeStruct((8, lanes), f32),
            jax.ShapeDtypeStruct((columns, lanes), jnp.bfloat16),
            jax.ShapeDtypeStruct((columns, lanes), f32),
            jax.ShapeDtypeStruct((buckets * LANE_ROWS, lanes), f32),
        ),
        in_specs=[any_spec()],
        out_specs=(vmem_spec(),) * 4,
        scratch_shapes=[pltpu.SemaphoreType.DMA((buckets,))],
        compiler_params=params,
        name="stats",
    )(in_hbm(logits.T))

    listed = (DEPTH, buckets * LANE_ROWS, lanes)
    compact = DEPTH * children + 8
    local, targets, index, share, value, flags, sums = pl.pallas_call(
        functools.partial(lists_kernel, groups, bucket, group),
        out_shape=(
            jax.ShapeDtypeStruct((children, lanes), jnp.int32),
            jax.ShapeDtypeStruct((children, lanes), f32),
            jax.ShapeDtypeStruct(listed, jnp.bfloat16),
            jax.ShapeDtypeStruct(listed, f32),
            jax.ShapeDtypeStruct(listed, jnp.bfloat16),
            jax.ShapeDtypeStruct((buckets,), jnp.int32),
            jax.ShapeDtypeStruct((8, lanes), f32),
        ),
        in_specs=[vmem_spec()] * (groups + 4),
        out_specs=(vmem_spec(),) * 5 + (smem_spec(), vmem_spec()),
        scratch_shapes=[
            pltpu.VMEM((children, lanes), jnp.int32),
            pltpu.VMEM((DEPTH, children, lanes), f32),
            pltpu.VMEM((compact, lanes), jnp.int32),
            pltpu.VMEM((compact, lanes), f32),
            pltpu.VMEM((compact, lanes), f32),
        ],
        compiler_params=params,
        name="lists",
    )(*routed, ids, stats, x, power)

    hop = 1
    while hop < shards:
        pairs = [(i, i ^ hop) for i in range(shards)]
        sums = merge(sums, lax.ppermute(sums, "tensor", pairs))
        hop *= 2
    lse = sums[0:1] + jnp.log(sums[1:2])
    own = lse - sums[2:3]
    others = shifted(own, "dp", groups)

    gradient, row_loss = pl.pallas_call(
        functools.partial(gradient_kernel, bucket),
        out_shape=(
            jax.ShapeDtypeStruct((columns, lanes), jnp.bfloat16),
            jax.ShapeDtypeStruct((1, lanes), f32),
        ),
        in_specs=[smem_spec()] + [vmem_spec()] * 9,
        out_specs=(any_spec(), any_spec()),
        scratch_shapes=[
            pltpu.VMEM((columns, lanes), jnp.bfloat16),
            pltpu.SemaphoreType.DMA((buckets,)),
            pltpu.SemaphoreType.DMA(()),
        ],
        compiler_params=params,
        name="gradient",
    )(flags, lse, own, local, targets, index, share, value, power, tops)
    losses = [own] + others
    while len(losses) > 1:
        losses = [losses[i] + losses[i + 1] for i in range(0, len(losses), 2)]
    mean_loss = jnp.sum(losses[0]) / (groups * lanes)
    return gradient.T, row_loss.reshape(lanes), mean_loss


def solution(mesh):
    return jax.shard_map(
        body,
        mesh=mesh,
        in_specs=(P("dp", "tensor"), P("dp", None), P("dp", None), P("dp"), P("dp"), P("dp")),
        out_specs=(P("dp", "tensor"), P("dp"), P()),
        check_vma=False,
    )
```

```python
import functools
import math

import jax
import jax.numpy as jnp
from jax import lax
from jax.experimental import pallas as pl
from jax.experimental.pallas import tpu as pltpu
from jax.sharding import PartitionSpec as P

LOG2E = 1.4426950408889634
LANE_ROWS = 16
DEPTH = 4
UNROLL = 4
CHAINS = 4
USUAL = 2
VMEM_BYTES = 13 * 1024 * 1024


def largest_block(rows, limit):
    units = rows // LANE_ROWS
    best = 1
    for size in range(1, units + 1):
        if units % size == 0 and size * LANE_ROWS <= limit:
            best = size
    return best * LANE_ROWS


def any_spec():
    return pl.BlockSpec(memory_space=pltpu.HBM)


def in_hbm(array):
    return pltpu.with_memory_space_constraint(array, pltpu.HBM)


def vmem_spec():
    return pl.BlockSpec(memory_space=pltpu.VMEM)


def smem_spec():
    return pl.BlockSpec(memory_space=pltpu.SMEM)


def prepare_kernel(counts_ref, valid_ref, temp_ref, owner_ref, out_ref):
    children, rows = counts_ref.shape
    slot = lax.broadcasted_iota(jnp.int32, (children, rows), 0)
    powered = jnp.exp(jnp.log(counts_ref[...].astype(jnp.float32)) * temp_ref[...])
    weights = jnp.where(slot < valid_ref[...], powered, 0.0)
    out_ref[:children, :] = weights / jnp.sum(weights, axis=0, keepdims=True)
    extra = out_ref.shape[0] - children
    out_ref[children:, :] = jnp.broadcast_to(owner_ref[...].astype(jnp.float32), (extra, rows))


def stats_kernel(block, x_hbm, out_ref, x_ref, power_ref, top_ref, sems):
    total, lanes = x_ref.shape
    blocks = total // block
    units = block // LANE_ROWS

    def copy(index):
        window = pl.ds(index * block, block)
        return pltpu.make_async_copy(x_hbm.at[window, :], x_ref.at[window, :], sems.at[index])

    for index in range(blocks):
        copy(index).start()

    def view(ref, index):
        return ref.at[pl.ds(pl.multiple_of(index * block, LANE_ROWS), block), :]

    def block_pass(index, wide, acc, following, best):
        top_ref[pl.ds(pl.multiple_of(index * LANE_ROWS, LANE_ROWS), LANE_ROWS), :] = wide
        x, powers = view(x_ref, index), view(power_ref, index)
        following = None if following is None else view(x_ref, following)
        tops = [best] * CHAINS
        for i in range(units):
            row = slice(i * LANE_ROWS, (i + 1) * LANE_ROWS)
            power = jnp.exp2((x[row, :].astype(jnp.float32) - wide) * LOG2E)
            powers[row, :] = power
            acc = acc + power
            if following is not None:
                tops[i % CHAINS] = jnp.maximum(tops[i % CHAINS], following[row, :])
        return acc, functools.reduce(jnp.maximum, tops)

    def one(index, carry):
        top, acc = carry
        copy(index + 1).wait()
        wide = top.astype(jnp.float32)
        acc, new_top = block_pass(index, wide, acc, index + 1, top)
        acc = acc * jnp.exp2((wide - new_top.astype(jnp.float32)) * LOG2E)
        return new_top, acc

    copy(0).wait()
    first = view(x_ref, 0)
    tops = [first[i * LANE_ROWS : (i + 1) * LANE_ROWS, :] for i in range(units)]
    top = functools.reduce(jnp.maximum, tops)
    top, acc = lax.fori_loop(0, blocks - 1, one, (top, jnp.zeros((LANE_ROWS, lanes), jnp.float32)))
    wide = top.astype(jnp.float32)
    acc, _ = block_pass(blocks - 1, wide, acc, None, top)
    row_top = jnp.max(wide, axis=0, keepdims=True)
    row_sum = jnp.sum(acc * jnp.exp2((wide - row_top) * LOG2E), axis=0, keepdims=True)
    out_ref[0:1, :] = row_top
    out_ref[1:2, :] = row_sum
    out_ref[2:, :] = jnp.zeros((out_ref.shape[0] - 2, lanes), jnp.float32)


def dense_rows(ids_ref, targets_ref, first_row, shape):
    row = lax.broadcasted_iota(jnp.int32, shape, 0) + first_row

    def add(j, dense):
        hit = ids_ref[pl.ds(j, 1), :] == row
        return dense + jnp.where(hit, targets_ref[pl.ds(j, 1), :], 0.0)

    return lax.fori_loop(0, ids_ref.shape[0], add, jnp.zeros(shape, jnp.float32))


def lists_kernel(leaf_blocks, bucket, group, *refs):
    routed = refs[:leaf_blocks]
    ids_ref, stats_ref, x_ref, _, *results = refs[leaf_blocks:]
    local_ref, targets_ref, index_ref, share_ref, value_ref, flag_ref, out_ref = results[:7]
    code_ref, rank_ref, slot_ref, at_ref, part_ref = results[7:]
    f32 = jnp.float32
    total, lanes = x_ref.shape
    children = ids_ref.shape[0]
    buckets = total // bucket
    groups = buckets // group
    units = bucket // LANE_ROWS
    slots = group * LANE_ROWS
    local = ids_ref[...] - lax.axis_index("tensor") * total
    local_ref[...] = local

    inside = (local >= 0) & (local < total)
    unit = local // LANE_ROWS
    at_bucket = ((unit.astype(f32) + 0.5) * (1.0 / units)).astype(jnp.int32)
    at = unit - at_bucket * units
    slot = at_bucket * LANE_ROWS + (local & (LANE_ROWS - 1))
    slot = jnp.where(inside, slot, -1)
    slot_ref[:children, :] = slot
    code_ref[...] = slot * 256 + at + 1

    tiles = children // 8
    sublane = lax.broadcasted_iota(jnp.int32, (8, lanes), 0)
    tile_slot = [slot[8 * t : 8 * t + 8] for t in range(tiles)]
    depth = [jnp.zeros((8, lanes), jnp.int32) for _ in range(tiles)]
    for j in range(children):
        row = slot_ref[j : j + 1, :]
        own = j // 8
        hit = (tile_slot[own] == row) & (sublane > j % 8)
        depth[own] = depth[own] + jnp.where(hit, 1, 0)
        for t in range(own + 1, tiles):
            depth[t] = depth[t] + jnp.where(tile_slot[t] == row, 1, 0)
    depth = jnp.where(inside, jnp.concatenate(depth, axis=0), -1)

    lower = lax.broadcasted_iota(jnp.int32, (children, children), 0)
    lower = lower > lax.broadcasted_iota(jnp.int32, (children, children), 1)
    lower = jnp.where(lower, 1.0, 0.0).astype(jnp.bfloat16)
    counts = []
    for k in range(DEPTH):
        chosen = jnp.where(depth == k, 1.0, 0.0)
        rank = jnp.dot(lower, chosen.astype(jnp.bfloat16), preferred_element_type=f32)
        rank_ref[k] = jnp.where(depth == k, rank, -1.0)
        counts.append(jnp.max(jnp.sum(chosen, axis=0, keepdims=True)).astype(jnp.int32))
    deepest = jnp.max(depth.astype(f32)).astype(jnp.int32)

    position = lax.broadcasted_iota(jnp.int32, (lanes, lanes), 0) + lax.axis_index("dp") * lanes
    parts = jnp.zeros((3 * children, lanes), f32)
    for block in routed:
        owner = block[children : children + 1, :].astype(jnp.int32)
        matcher = jnp.where(owner == position, 1.0, 0.0).astype(jnp.bfloat16)
        rest = block[:children, :]
        pieces = []
        for _ in range(3):
            piece = rest.astype(jnp.bfloat16)
            pieces.append(piece)
            rest = rest - piece.astype(f32)
        stacked = jnp.concatenate(pieces, axis=0)
        parts = parts + lax.dot_general(
            stacked, matcher, (((1,), (1,)), ((), ())), preferred_element_type=f32
        )
    targets_ref[...] = parts[:children] + parts[children : 2 * children] + parts[2 * children :]

    for b in range(buckets):
        flag_ref[b] = 0

    @pl.when(deepest >= USUAL)
    def _():
        for b in range(buckets):
            most = jnp.max(jnp.where(at_bucket == b, depth, -1).astype(f32)).astype(jnp.int32)
            deeper = jnp.where(most >= USUAL, 1, 0).astype(jnp.int32)
            flag_ref[b] = jnp.where(most >= DEPTH, 2, deeper).astype(jnp.int32)

    steps = [(count + UNROLL - 1) // UNROLL for count in counts]
    for k in range(DEPTH):

        def compact(step, unused, k=k):
            for u in range(UNROLL):
                r = step * UNROLL + u
                hit = rank_ref[k] == r.astype(f32)
                code = jnp.sum(jnp.where(hit, code_ref[...], 0), axis=0, keepdims=True) - 1
                part = jnp.sum(jnp.where(hit, targets_ref[...], 0.0), axis=0, keepdims=True)
                row = pl.ds(k * children + r, 1)
                slot_ref[row, :] = code >> 8
                at_ref[row, :] = (code & 255).astype(f32)
                part_ref[row, :] = part
            return unused

        lax.fori_loop(0, steps[k], compact, 0)

    def fill(g, unused, levels):
        slot_row = lax.broadcasted_iota(jnp.int32, (slots, lanes), 0) + g * slots
        rows = pl.ds(pl.multiple_of(g * slots, LANE_ROWS), slots)
        index = [index_ref[k, rows, :].astype(f32) for k in range(levels[0])]
        share = [share_ref[k, rows, :] for k in range(levels[0])]
        for k in levels:

            def add(step, carry, k=k):
                found, amount = carry
                for u in range(UNROLL):
                    row = pl.ds(k * children + step * UNROLL + u, 1)
                    hit = slot_ref[row, :] == slot_row
                    found = jnp.where(hit, at_ref[row, :], found)
                    amount = jnp.where(hit, part_ref[row, :], amount)
                return found, amount

            none = jnp.full((slots, lanes), -1.0, f32)
            zero = jnp.zeros((slots, lanes), f32)
            found, amount = lax.fori_loop(0, steps[k], add, (none, zero))
            for earlier in range(k):
                same = index[earlier] == found
                share[earlier] = share[earlier] + jnp.where(same, amount, 0.0)
                found = jnp.where(same, -1.0, found)
                amount = jnp.where(same, 0.0, amount)
            index.append(found)
            share.append(amount)
        for k in range(levels[-1] + 1):
            if k in levels:
                index_ref[k, rows, :] = index[k].astype(jnp.bfloat16)
            share_ref[k, rows, :] = share[k]
        return unused

    lax.fori_loop(0, groups, functools.partial(fill, levels=tuple(range(USUAL))), 0)

    @pl.when(deepest >= USUAL)
    def _():
        def deepen(g, unused):
            flags = [flag_ref[g * group + b] for b in range(group)]

            @pl.when(sum(flags) > 0)
            def _():
                fill(g, 0, tuple(range(USUAL, DEPTH)))

            return unused

        lax.fori_loop(0, groups, deepen, 0)

    out_ref[...] = stats_ref[...]

    def pick(b, picked):
        base = pl.multiple_of(b * bucket, LANE_ROWS)
        at_rows = pl.ds(pl.multiple_of(b * LANE_ROWS, LANE_ROWS), LANE_ROWS)

        def fast(entries):
            index = [index_ref[k, at_rows, :] for k in range(entries)]
            found = [jnp.zeros((LANE_ROWS, lanes), jnp.bfloat16)] * entries
            x = x_ref.at[pl.ds(base, bucket), :]
            for i in range(units):
                values = x[i * LANE_ROWS : (i + 1) * LANE_ROWS, :]
                mark = jnp.bfloat16(i)
                found = [jnp.where(index[k] == mark, values, found[k]) for k in range(entries)]
            extra = jnp.zeros((LANE_ROWS, lanes), f32)
            for k in range(entries):
                value_ref[k, at_rows, :] = found[k]
                extra = extra + share_ref[k, at_rows, :] * found[k].astype(f32)
            return extra

        def slow():
            def add(i, extra):
                row = pl.multiple_of(base + i * LANE_ROWS, LANE_ROWS)
                dense = dense_rows(local_ref, targets_ref, row, (LANE_ROWS, lanes))
                values = x_ref[pl.ds(row, LANE_ROWS), :].astype(f32)
                return extra + dense * values

            zero = jnp.zeros((LANE_ROWS, lanes), f32)
            for k in range(DEPTH):
                value_ref[k, at_rows, :] = zero.astype(jnp.bfloat16)
            return lax.fori_loop(0, units, add, zero)

        usual = functools.partial(fast, USUAL)
        deeper = functools.partial(fast, DEPTH)
        rare = lambda: lax.cond(flag_ref[b] == 1, deeper, slow)
        return picked + lax.cond(flag_ref[b] == 0, usual, rare)

    picked = lax.fori_loop(0, buckets, pick, jnp.zeros((LANE_ROWS, lanes), f32))
    out_ref[2:3, :] = jnp.sum(picked, axis=0, keepdims=True)


def gradient_kernel(
    bucket,
    flag_ref,
    lse_ref,
    own_ref,
    local_ref,
    targets_ref,
    index_ref,
    share_ref,
    value_ref,
    power_ref,
    top_ref,
    out_hbm,
    loss_hbm,
    out_ref,
    sems,
    loss_sem,
):
    total, lanes = power_ref.shape
    buckets = total // bucket

    def back(index):
        window = pl.ds(index * bucket, bucket)
        return pltpu.make_async_copy(out_ref.at[window, :], out_hbm.at[window, :], sems.at[index])

    losses = pltpu.make_async_copy(own_ref, loss_hbm, loss_sem)
    losses.start()
    lse = jnp.broadcast_to(lse_ref[0:1, :], (LANE_ROWS, lanes))

    def one(b, carry):
        base = pl.multiple_of(b * bucket, LANE_ROWS)
        at = pl.ds(pl.multiple_of(b * LANE_ROWS, LANE_ROWS), LANE_ROWS)
        scale = jnp.exp2((top_ref[at, :] - lse) * LOG2E)

        def listed(entries):
            index = [index_ref[k, at, :] for k in range(entries)]
            given = []
            for k in range(entries):
                value = value_ref[k, at, :].astype(jnp.float32)
                soft = jnp.exp2((value - lse) * LOG2E)
                given.append((soft - share_ref[k, at, :]).astype(jnp.bfloat16))
            powers = power_ref.at[pl.ds(base, bucket), :]
            results = out_ref.at[pl.ds(base, bucket), :]
            for i in range(bucket // LANE_ROWS):
                row = slice(i * LANE_ROWS, (i + 1) * LANE_ROWS)
                result = (powers[row, :] * scale).astype(jnp.bfloat16)
                mark = jnp.bfloat16(i)
                for k in range(entries):
                    result = jnp.where(index[k] == mark, given[k], result)
                results[row, :] = result

        pl.when(flag_ref[b] == 0)(functools.partial(listed, USUAL))
        pl.when(flag_ref[b] == 1)(functools.partial(listed, DEPTH))

        @pl.when(flag_ref[b] == 2)
        def _():
            def fill(i, unused):
                first = pl.multiple_of(base + i * LANE_ROWS, LANE_ROWS)
                dense = dense_rows(local_ref, targets_ref, first, (LANE_ROWS, lanes))
                row = pl.ds(first, LANE_ROWS)
                out_ref[row, :] = (power_ref[row, :] * scale - dense).astype(jnp.bfloat16)
                return unused

            lax.fori_loop(0, bucket // LANE_ROWS, fill, 0)

        back(b).start()
        return carry

    lax.fori_loop(0, buckets, one, 0)
    for index in range(buckets):
        back(index).wait()
    losses.wait()


def shifted(value, axis, size):
    result = []
    for shift in range(1, size):
        pairs = [(i, i ^ shift) for i in range(size)]
        result.append(lax.ppermute(value, axis, pairs))
    return result


def merge(one, other):
    top = jnp.maximum(one[0:1], other[0:1])
    total = one[1:2] * jnp.exp(one[0:1] - top) + other[1:2] * jnp.exp(other[0:1] - top)
    picked = one[2:3] + other[2:3]
    return jnp.concatenate([top, total, picked, jnp.zeros_like(one[3:])], axis=0)


def body(logits, child_ids, leaf_counts, leaf_valid, leaf_temp, leaf_owner):
    lanes, columns = logits.shape
    children = child_ids.shape[1]
    groups = lax.axis_size("dp")
    shards = lax.axis_size("tensor")
    f32 = jnp.float32
    params = pltpu.CompilerParams(vmem_limit_bytes=VMEM_BYTES)
    ids = child_ids.T

    leaf = pl.pallas_call(
        prepare_kernel,
        out_shape=jax.ShapeDtypeStruct((children + 8, lanes), f32),
        compiler_params=params,
        name="prepare",
    )(
        in_hbm(leaf_counts.T),
        in_hbm(leaf_valid.reshape(1, lanes)),
        in_hbm(leaf_temp.reshape(1, lanes)),
        in_hbm(leaf_owner.reshape(1, lanes)),
    )
    routed = [leaf] + shifted(leaf, "dp", groups)

    bucket = largest_block(columns, 1584)
    buckets = columns // bucket
    group = 3 if buckets % 3 == 0 else 1
    stats, x, power, tops = pl.pallas_call(
        functools.partial(stats_kernel, bucket),
        out_shape=(
            jax.ShapeDtypeStruct((8, lanes), f32),
            jax.ShapeDtypeStruct((columns, lanes), jnp.bfloat16),
            jax.ShapeDtypeStruct((columns, lanes), f32),
            jax.ShapeDtypeStruct((buckets * LANE_ROWS, lanes), f32),
        ),
        in_specs=[any_spec()],
        out_specs=(vmem_spec(),) * 4,
        scratch_shapes=[pltpu.SemaphoreType.DMA((buckets,))],
        compiler_params=params,
        name="stats",
    )(in_hbm(logits.T))

    listed = (DEPTH, buckets * LANE_ROWS, lanes)
    compact = DEPTH * children + 8
    local, targets, index, share, value, flags, sums = pl.pallas_call(
        functools.partial(lists_kernel, groups, bucket, group),
        out_shape=(
            jax.ShapeDtypeStruct((children, lanes), jnp.int32),
            jax.ShapeDtypeStruct((children, lanes), f32),
            jax.ShapeDtypeStruct(listed, jnp.bfloat16),
            jax.ShapeDtypeStruct(listed, f32),
            jax.ShapeDtypeStruct(listed, jnp.bfloat16),
            jax.ShapeDtypeStruct((buckets,), jnp.int32),
            jax.ShapeDtypeStruct((8, lanes), f32),
        ),
        in_specs=[vmem_spec()] * (groups + 4),
        out_specs=(vmem_spec(),) * 5 + (smem_spec(), vmem_spec()),
        scratch_shapes=[
            pltpu.VMEM((children, lanes), jnp.int32),
            pltpu.VMEM((DEPTH, children, lanes), f32),
            pltpu.VMEM((compact, lanes), jnp.int32),
            pltpu.VMEM((compact, lanes), f32),
            pltpu.VMEM((compact, lanes), f32),
        ],
        compiler_params=params,
        name="lists",
    )(*routed, ids, stats, x, power)

    hop = 1
    while hop < shards:
        pairs = [(i, i ^ hop) for i in range(shards)]
        sums = merge(sums, lax.ppermute(sums, "tensor", pairs))
        hop *= 2
    lse = sums[0:1] + jnp.log(sums[1:2])
    own = lse - sums[2:3]
    portion = own / (groups * lanes)
    others = shifted(portion, "dp", groups)

    gradient, row_loss = pl.pallas_call(
        functools.partial(gradient_kernel, bucket),
        out_shape=(
            jax.ShapeDtypeStruct((columns, lanes), jnp.bfloat16),
            jax.ShapeDtypeStruct((1, lanes), f32),
        ),
        in_specs=[smem_spec()] + [vmem_spec()] * 9,
        out_specs=(any_spec(), any_spec()),
        scratch_shapes=[
            pltpu.VMEM((columns, lanes), jnp.bfloat16),
            pltpu.SemaphoreType.DMA((buckets,)),
            pltpu.SemaphoreType.DMA(()),
        ],
        compiler_params=params,
        name="gradient",
    )(flags, lse, own, local, targets, index, share, value, power, tops)
    losses = [portion] + others
    while len(losses) > 1:
        losses = [losses[i] + losses[i + 1] for i in range(0, len(losses), 2)]
    mean_loss = jnp.sum(losses[0])
    return gradient.T, row_loss.reshape(lanes), mean_loss


def solution(mesh):
    return jax.shard_map(
        body,
        mesh=mesh,
        in_specs=(P("dp", "tensor"), P("dp", None), P("dp", None), P("dp"), P("dp"), P("dp")),
        out_specs=(P("dp", "tensor"), P("dp"), P()),
        check_vma=False,
    )
```

```python
import functools
import math

import jax
import jax.numpy as jnp
from jax import lax
from jax.experimental import pallas as pl
from jax.experimental.pallas import tpu as pltpu
from jax.sharding import PartitionSpec as P

LOG2E = 1.4426950408889634
LANE_ROWS = 16
DEPTH = 4
UNROLL = 4
CHAINS = 4
PIECES = 3
USUAL = 2
VMEM_BYTES = 13 * 1024 * 1024


def largest_block(rows, limit):
    units = rows // LANE_ROWS
    best = 1
    for size in range(1, units + 1):
        if units % size == 0 and size * LANE_ROWS <= limit:
            best = size
    return best * LANE_ROWS


def any_spec():
    return pl.BlockSpec(memory_space=pltpu.HBM)


def in_hbm(array):
    return pltpu.with_memory_space_constraint(array, pltpu.HBM)


def vmem_spec():
    return pl.BlockSpec(memory_space=pltpu.VMEM)


def smem_spec():
    return pl.BlockSpec(memory_space=pltpu.SMEM)


def prepare_kernel(counts_ref, valid_ref, temp_ref, owner_ref, out_ref):
    children, rows = counts_ref.shape
    slot = lax.broadcasted_iota(jnp.int32, (children, rows), 0)
    powered = jnp.exp(jnp.log(counts_ref[...].astype(jnp.float32)) * temp_ref[...])
    weights = jnp.where(slot < valid_ref[...], powered, 0.0)
    out_ref[:children, :] = weights / jnp.sum(weights, axis=0, keepdims=True)
    extra = out_ref.shape[0] - children
    out_ref[children:, :] = jnp.broadcast_to(owner_ref[...].astype(jnp.float32), (extra, rows))


def stats_kernel(block, x_hbm, out_ref, x_ref, power_ref, top_ref, sems):
    total, lanes = x_ref.shape
    blocks = total // block
    units = block // LANE_ROWS

    def copy(index):
        window = pl.ds(index * block, block)
        return pltpu.make_async_copy(x_hbm.at[window, :], x_ref.at[window, :], sems.at[index])

    for index in range(blocks):
        copy(index).start()

    def view(ref, index):
        return ref.at[pl.ds(pl.multiple_of(index * block, LANE_ROWS), block), :]

    def block_pass(index, wide, acc, following, best):
        top_ref[pl.ds(pl.multiple_of(index * LANE_ROWS, LANE_ROWS), LANE_ROWS), :] = wide
        x, powers = view(x_ref, index), view(power_ref, index)
        following = None if following is None else view(x_ref, following)
        tops = [best] * CHAINS
        for i in range(units):
            row = slice(i * LANE_ROWS, (i + 1) * LANE_ROWS)
            power = jnp.exp2((x[row, :].astype(jnp.float32) - wide) * LOG2E)
            powers[row, :] = power
            acc = acc + power
            if following is not None:
                tops[i % CHAINS] = jnp.maximum(tops[i % CHAINS], following[row, :])
        return acc, functools.reduce(jnp.maximum, tops)

    def one(index, carry):
        top, acc = carry
        copy(index + 1).wait()
        wide = top.astype(jnp.float32)
        acc, new_top = block_pass(index, wide, acc, index + 1, top)
        acc = acc * jnp.exp2((wide - new_top.astype(jnp.float32)) * LOG2E)
        return new_top, acc

    copy(0).wait()
    first = view(x_ref, 0)
    tops = [first[i * LANE_ROWS : (i + 1) * LANE_ROWS, :] for i in range(units)]
    chains = tops[:CHAINS]
    for i in range(CHAINS, units):
        chains[i % CHAINS] = jnp.maximum(chains[i % CHAINS], tops[i])
    top = functools.reduce(jnp.maximum, chains)
    top, acc = lax.fori_loop(0, blocks - 1, one, (top, jnp.zeros((LANE_ROWS, lanes), jnp.float32)))
    wide = top.astype(jnp.float32)
    acc, _ = block_pass(blocks - 1, wide, acc, None, top)
    row_top = jnp.max(wide, axis=0, keepdims=True)
    row_sum = jnp.sum(acc * jnp.exp2((wide - row_top) * LOG2E), axis=0, keepdims=True)
    out_ref[0:1, :] = row_top
    out_ref[1:2, :] = row_sum
    out_ref[2:, :] = jnp.zeros((out_ref.shape[0] - 2, lanes), jnp.float32)


def dense_rows(ids_ref, targets_ref, first_row, shape):
    row = lax.broadcasted_iota(jnp.int32, shape, 0) + first_row

    def add(j, dense):
        hit = ids_ref[pl.ds(j, 1), :] == row
        return dense + jnp.where(hit, targets_ref[pl.ds(j, 1), :], 0.0)

    return lax.fori_loop(0, ids_ref.shape[0], add, jnp.zeros(shape, jnp.float32))


def lists_kernel(leaf_blocks, bucket, group, *refs):
    routed = refs[:leaf_blocks]
    ids_ref, stats_ref, x_ref, _, *results = refs[leaf_blocks:]
    local_ref, targets_ref, index_ref, share_ref, value_ref, flag_ref, out_ref = results[:7]
    code_ref, rank_ref, slot_ref, at_ref, part_ref = results[7:]
    f32 = jnp.float32
    total, lanes = x_ref.shape
    children = ids_ref.shape[0]
    buckets = total // bucket
    groups = buckets // group
    units = bucket // LANE_ROWS
    slots = group * LANE_ROWS
    local = ids_ref[...] - lax.axis_index("tensor") * total
    local_ref[...] = local

    inside = (local >= 0) & (local < total)
    unit = local // LANE_ROWS
    at_bucket = ((unit.astype(f32) + 0.5) * (1.0 / units)).astype(jnp.int32)
    at = unit - at_bucket * units
    slot = at_bucket * LANE_ROWS + (local & (LANE_ROWS - 1))
    slot = jnp.where(inside, slot, -1)
    slot_ref[:children, :] = slot
    code_ref[...] = slot * 256 + at + 1

    tiles = children // 8
    sublane = lax.broadcasted_iota(jnp.int32, (8, lanes), 0)
    tile_slot = [slot[8 * t : 8 * t + 8] for t in range(tiles)]
    depth = [jnp.zeros((8, lanes), jnp.int32) for _ in range(tiles)]
    for j in range(children):
        row = slot_ref[j : j + 1, :]
        own = j // 8
        hit = (tile_slot[own] == row) & (sublane > j % 8)
        depth[own] = depth[own] + jnp.where(hit, 1, 0)
        for t in range(own + 1, tiles):
            depth[t] = depth[t] + jnp.where(tile_slot[t] == row, 1, 0)
    depth = jnp.where(inside, jnp.concatenate(depth, axis=0), -1)

    lower = lax.broadcasted_iota(jnp.int32, (children, children), 0)
    lower = lower > lax.broadcasted_iota(jnp.int32, (children, children), 1)
    lower = jnp.where(lower, 1.0, 0.0).astype(jnp.bfloat16)
    counts = []
    for k in range(DEPTH):
        chosen = jnp.where(depth == k, 1.0, 0.0)
        rank = jnp.dot(lower, chosen.astype(jnp.bfloat16), preferred_element_type=f32)
        rank_ref[k] = jnp.where(depth == k, rank, -1.0)
        counts.append(jnp.max(jnp.sum(chosen, axis=0, keepdims=True)).astype(jnp.int32))
    deepest = jnp.max(depth.astype(f32)).astype(jnp.int32)

    position = lax.broadcasted_iota(jnp.int32, (lanes, lanes), 0) + lax.axis_index("dp") * lanes
    parts = jnp.zeros((3 * children, lanes), f32)
    for block in routed:
        owner = block[children : children + 1, :].astype(jnp.int32)
        matcher = jnp.where(owner == position, 1.0, 0.0).astype(jnp.bfloat16)
        rest = block[:children, :]
        pieces = []
        for _ in range(3):
            piece = rest.astype(jnp.bfloat16)
            pieces.append(piece)
            rest = rest - piece.astype(f32)
        stacked = jnp.concatenate(pieces, axis=0)
        parts = parts + lax.dot_general(
            stacked, matcher, (((1,), (1,)), ((), ())), preferred_element_type=f32
        )
    targets_ref[...] = parts[:children] + parts[children : 2 * children] + parts[2 * children :]

    for b in range(buckets):
        flag_ref[b] = 0

    @pl.when(deepest >= USUAL)
    def _():
        for b in range(buckets):
            most = jnp.max(jnp.where(at_bucket == b, depth, -1).astype(f32)).astype(jnp.int32)
            deeper = jnp.where(most >= USUAL, 1, 0).astype(jnp.int32)
            flag_ref[b] = jnp.where(most >= DEPTH, 2, deeper).astype(jnp.int32)

    steps = [(count + UNROLL - 1) // UNROLL for count in counts]
    for k in range(DEPTH):

        def compact(step, unused, k=k):
            for u in range(UNROLL):
                r = step * UNROLL + u
                hit = rank_ref[k] == r.astype(f32)
                code = jnp.sum(jnp.where(hit, code_ref[...], 0), axis=0, keepdims=True) - 1
                part = jnp.sum(jnp.where(hit, targets_ref[...], 0.0), axis=0, keepdims=True)
                row = pl.ds(k * children + r, 1)
                slot_ref[row, :] = code >> 8
                at_ref[row, :] = (code & 255).astype(f32)
                part_ref[row, :] = part
            return unused

        lax.fori_loop(0, steps[k], compact, 0)

    def fill(g, unused, levels):
        slot_row = lax.broadcasted_iota(jnp.int32, (slots, lanes), 0) + g * slots
        rows = pl.ds(pl.multiple_of(g * slots, LANE_ROWS), slots)
        index = [index_ref[k, rows, :].astype(f32) for k in range(levels[0])]
        share = [share_ref[k, rows, :] for k in range(levels[0])]
        for k in levels:

            def add(step, carry, k=k):
                found, amount = carry
                for u in range(UNROLL):
                    row = pl.ds(k * children + step * UNROLL + u, 1)
                    hit = slot_ref[row, :] == slot_row
                    found = jnp.where(hit, at_ref[row, :], found)
                    amount = jnp.where(hit, part_ref[row, :], amount)
                return found, amount

            none = jnp.full((slots, lanes), -1.0, f32)
            zero = jnp.zeros((slots, lanes), f32)
            found, amount = lax.fori_loop(0, steps[k], add, (none, zero))
            for earlier in range(k):
                same = index[earlier] == found
                share[earlier] = share[earlier] + jnp.where(same, amount, 0.0)
                found = jnp.where(same, -1.0, found)
                amount = jnp.where(same, 0.0, amount)
            index.append(found)
            share.append(amount)
        for k in range(levels[-1] + 1):
            if k in levels:
                index_ref[k, rows, :] = index[k].astype(jnp.bfloat16)
            share_ref[k, rows, :] = share[k]
        return unused

    lax.fori_loop(0, groups, functools.partial(fill, levels=tuple(range(USUAL))), 0)

    @pl.when(deepest >= USUAL)
    def _():
        def deepen(g, unused):
            flags = [flag_ref[g * group + b] for b in range(group)]

            @pl.when(sum(flags) > 0)
            def _():
                fill(g, 0, tuple(range(USUAL, DEPTH)))

            return unused

        lax.fori_loop(0, groups, deepen, 0)

    out_ref[...] = stats_ref[...]

    def pick(b, picked):
        base = pl.multiple_of(b * bucket, LANE_ROWS)
        at_rows = pl.ds(pl.multiple_of(b * LANE_ROWS, LANE_ROWS), LANE_ROWS)

        def fast(entries):
            index = [index_ref[k, at_rows, :] for k in range(entries)]
            found = [jnp.zeros((LANE_ROWS, lanes), jnp.bfloat16)] * entries
            x = x_ref.at[pl.ds(base, bucket), :]
            for i in range(units):
                values = x[i * LANE_ROWS : (i + 1) * LANE_ROWS, :]
                mark = jnp.bfloat16(i)
                found = [jnp.where(index[k] == mark, values, found[k]) for k in range(entries)]
            extra = jnp.zeros((LANE_ROWS, lanes), f32)
            for k in range(entries):
                value_ref[k, at_rows, :] = found[k]
                extra = extra + share_ref[k, at_rows, :] * found[k].astype(f32)
            return extra

        def slow():
            def add(i, extra):
                row = pl.multiple_of(base + i * LANE_ROWS, LANE_ROWS)
                dense = dense_rows(local_ref, targets_ref, row, (LANE_ROWS, lanes))
                values = x_ref[pl.ds(row, LANE_ROWS), :].astype(f32)
                return extra + dense * values

            zero = jnp.zeros((LANE_ROWS, lanes), f32)
            for k in range(DEPTH):
                value_ref[k, at_rows, :] = zero.astype(jnp.bfloat16)
            return lax.fori_loop(0, units, add, zero)

        usual = functools.partial(fast, USUAL)
        deeper = functools.partial(fast, DEPTH)
        rare = lambda: lax.cond(flag_ref[b] == 1, deeper, slow)
        return picked + lax.cond(flag_ref[b] == 0, usual, rare)

    picked = lax.fori_loop(0, buckets, pick, jnp.zeros((LANE_ROWS, lanes), f32))
    out_ref[2:3, :] = jnp.sum(picked, axis=0, keepdims=True)


def gradient_kernel(
    bucket,
    flag_ref,
    lse_ref,
    own_ref,
    local_ref,
    targets_ref,
    index_ref,
    share_ref,
    value_ref,
    power_ref,
    top_ref,
    out_hbm,
    loss_hbm,
    out_ref,
    sems,
    loss_sem,
):
    total, lanes = power_ref.shape
    buckets = total // bucket

    units = bucket // LANE_ROWS
    pieces = PIECES if units % PIECES == 0 else 1
    piece = bucket // pieces

    def back(index):
        window = pl.ds(index * piece, piece)
        return pltpu.make_async_copy(out_ref.at[window, :], out_hbm.at[window, :], sems.at[index])

    losses = pltpu.make_async_copy(own_ref, loss_hbm, loss_sem)
    losses.start()
    lse = jnp.broadcast_to(lse_ref[0:1, :], (LANE_ROWS, lanes))

    def one(b, carry):
        base = pl.multiple_of(b * bucket, LANE_ROWS)
        at = pl.ds(pl.multiple_of(b * LANE_ROWS, LANE_ROWS), LANE_ROWS)
        scale = jnp.exp2((top_ref[at, :] - lse) * LOG2E)

        def listed(entries):
            index = [index_ref[k, at, :] for k in range(entries)]
            given = []
            for k in range(entries):
                value = value_ref[k, at, :].astype(jnp.float32)
                soft = jnp.exp2((value - lse) * LOG2E)
                given.append((soft - share_ref[k, at, :]).astype(jnp.bfloat16))
            powers = power_ref.at[pl.ds(base, bucket), :]
            results = out_ref.at[pl.ds(base, bucket), :]
            for i in range(units):
                row = slice(i * LANE_ROWS, (i + 1) * LANE_ROWS)
                result = (powers[row, :] * scale).astype(jnp.bfloat16)
                mark = jnp.bfloat16(i)
                for k in range(entries):
                    result = jnp.where(index[k] == mark, given[k], result)
                results[row, :] = result
                if (i + 1) % (units // pieces) == 0:
                    back(b * pieces + i // (units // pieces)).start()

        pl.when(flag_ref[b] == 0)(functools.partial(listed, USUAL))
        pl.when(flag_ref[b] == 1)(functools.partial(listed, DEPTH))

        @pl.when(flag_ref[b] == 2)
        def _():
            def fill(i, unused):
                first = pl.multiple_of(base + i * LANE_ROWS, LANE_ROWS)
                dense = dense_rows(local_ref, targets_ref, first, (LANE_ROWS, lanes))
                row = pl.ds(first, LANE_ROWS)
                out_ref[row, :] = (power_ref[row, :] * scale - dense).astype(jnp.bfloat16)
                return unused

            lax.fori_loop(0, units, fill, 0)
            for part in range(pieces):
                back(b * pieces + part).start()

        return carry

    lax.fori_loop(0, buckets, one, 0)
    for index in range(buckets * pieces):
        back(index).wait()
    losses.wait()


def shifted(value, axis, size):
    result = []
    for shift in range(1, size):
        pairs = [(i, i ^ shift) for i in range(size)]
        result.append(lax.ppermute(value, axis, pairs))
    return result


def merge(one, other):
    top = jnp.maximum(one[0:1], other[0:1])
    total = one[1:2] * jnp.exp(one[0:1] - top) + other[1:2] * jnp.exp(other[0:1] - top)
    picked = one[2:3] + other[2:3]
    return jnp.concatenate([top, total, picked, jnp.zeros_like(one[3:])], axis=0)


def body(logits, child_ids, leaf_counts, leaf_valid, leaf_temp, leaf_owner):
    lanes, columns = logits.shape
    children = child_ids.shape[1]
    groups = lax.axis_size("dp")
    shards = lax.axis_size("tensor")
    f32 = jnp.float32
    params = pltpu.CompilerParams(vmem_limit_bytes=VMEM_BYTES)
    ids = child_ids.T

    leaf = pl.pallas_call(
        prepare_kernel,
        out_shape=jax.ShapeDtypeStruct((children + 8, lanes), f32),
        compiler_params=params,
        name="prepare",
    )(
        in_hbm(leaf_counts.T),
        in_hbm(leaf_valid.reshape(1, lanes)),
        in_hbm(leaf_temp.reshape(1, lanes)),
        in_hbm(leaf_owner.reshape(1, lanes)),
    )
    routed = [leaf] + shifted(leaf, "dp", groups)

    bucket = largest_block(columns, 1584)
    buckets = columns // bucket
    group = 3 if buckets % 3 == 0 else 1
    stats, x, power, tops = pl.pallas_call(
        functools.partial(stats_kernel, bucket),
        out_shape=(
            jax.ShapeDtypeStruct((8, lanes), f32),
            jax.ShapeDtypeStruct((columns, lanes), jnp.bfloat16),
            jax.ShapeDtypeStruct((columns, lanes), f32),
            jax.ShapeDtypeStruct((buckets * LANE_ROWS, lanes), f32),
        ),
        in_specs=[any_spec()],
        out_specs=(vmem_spec(),) * 4,
        scratch_shapes=[pltpu.SemaphoreType.DMA((buckets,))],
        compiler_params=params,
        name="stats",
    )(in_hbm(logits.T))

    listed = (DEPTH, buckets * LANE_ROWS, lanes)
    compact = DEPTH * children + 8
    local, targets, index, share, value, flags, sums = pl.pallas_call(
        functools.partial(lists_kernel, groups, bucket, group),
        out_shape=(
            jax.ShapeDtypeStruct((children, lanes), jnp.int32),
            jax.ShapeDtypeStruct((children, lanes), f32),
            jax.ShapeDtypeStruct(listed, jnp.bfloat16),
            jax.ShapeDtypeStruct(listed, f32),
            jax.ShapeDtypeStruct(listed, jnp.bfloat16),
            jax.ShapeDtypeStruct((buckets,), jnp.int32),
            jax.ShapeDtypeStruct((8, lanes), f32),
        ),
        in_specs=[vmem_spec()] * (groups + 4),
        out_specs=(vmem_spec(),) * 5 + (smem_spec(), vmem_spec()),
        scratch_shapes=[
            pltpu.VMEM((children, lanes), jnp.int32),
            pltpu.VMEM((DEPTH, children, lanes), f32),
            pltpu.VMEM((compact, lanes), jnp.int32),
            pltpu.VMEM((compact, lanes), f32),
            pltpu.VMEM((compact, lanes), f32),
        ],
        compiler_params=params,
        name="lists",
    )(*routed, ids, stats, x, power)

    hop = 1
    while hop < shards:
        pairs = [(i, i ^ hop) for i in range(shards)]
        sums = merge(sums, lax.ppermute(sums, "tensor", pairs))
        hop *= 2
    lse = sums[0:1] + jnp.log(sums[1:2])
    own = lse - sums[2:3]
    portion = own / (groups * lanes)
    others = shifted(portion, "dp", groups)

    gradient, row_loss = pl.pallas_call(
        functools.partial(gradient_kernel, bucket),
        out_shape=(
            jax.ShapeDtypeStruct((columns, lanes), jnp.bfloat16),
            jax.ShapeDtypeStruct((1, lanes), f32),
        ),
        in_specs=[smem_spec()] + [vmem_spec()] * 9,
        out_specs=(any_spec(), any_spec()),
        scratch_shapes=[
            pltpu.VMEM((columns, lanes), jnp.bfloat16),
            pltpu.SemaphoreType.DMA((buckets * PIECES,)),
            pltpu.SemaphoreType.DMA(()),
        ],
        compiler_params=params,
        name="gradient",
    )(flags, lse, own, local, targets, index, share, value, power, tops)
    losses = [portion] + others
    while len(losses) > 1:
        losses = [losses[i] + losses[i + 1] for i in range(0, len(losses), 2)]
    mean_loss = jnp.sum(losses[0])
    return gradient.T, row_loss.reshape(lanes), mean_loss


def solution(mesh):
    return jax.shard_map(
        body,
        mesh=mesh,
        in_specs=(P("dp", "tensor"), P("dp", None), P("dp", None), P("dp"), P("dp"), P("dp")),
        out_specs=(P("dp", "tensor"), P("dp"), P()),
        check_vma=False,
    )
```
